512 devices in a mesh: grp: 2 (over y), ep: 16 (over z), tp: 8 (over x), mb: 2 (over core).
Axes of the slice: x: 8, y: 2, z: 16, core: 2. Of those that a mesh axis runs over, the one named last changes fastest.
The devices are a block of a 8x8x16 slice.
Arguments:
- hidden: bfloat16 [1024, 3584], P(('grp', 'ep', 'mb'), 'tp'), parts along dimension 0, may hold values from -12 to 12
- moe_gain: float32 [3584], P('tp'), may hold values from 0.1 to 1.9
- expert_ids: int32 [1024, 8], P(('grp', 'ep', 'mb')), parts along dimension 0, may hold values from 0 to 31, as said below
- slots: int32 [1024, 8], P(('grp', 'ep', 'mb')), parts along dimension 0, may hold values from 0 to 15, as said below
- affinity: float32 [1024, 8], P(('grp', 'ep', 'mb')), parts along dimension 0, may hold values from 0.05 to 1
- w_gate: bfloat16 [32, 3584, 1024], P(('ep', 'mb'), None, 'tp'), may hold values from -0.09375 to 0.09375
- w_up: bfloat16 [32, 3584, 1024], P(('ep', 'mb'), None, 'tp'), may hold values from -0.09375 to 0.09375
- w_down: bfloat16 [32, 1024, 3584], P(('ep', 'mb'), 'tp'), may hold values from -0.1875 to 0.1875
- attn_gain: float32 [3584], P('tp'), may hold values from 0.1 to 1.9
- w_dkv: bfloat16 [3584, 576], P('tp'), may hold values from -0.09375 to 0.09375
- kv_gain: float32 [512], replicated, may hold values from 0.1 to 1.9
- queries: bfloat16 [1024, 64, 576], P(('grp', 'ep', 'mb'), 'tp'), parts along dimension 0, may hold values from -36 to 36
- cache: bfloat16 [1024, 128, 576], P(('grp', 'ep', 'mb'), 'tp'), parts along dimension 0, may hold values from -4 to 4
- lengths: int32 [1024], P(('grp', 'ep', 'mb')), parts along dimension 0, may hold values from 2 to 128
Outputs:
- next_hidden: bfloat16 [1024, 3584], P(('grp', 'ep', 'mb'), 'tp'), parts along dimension 0
- latent_out: bfloat16 [1024, 64, 512], P(('grp', 'ep', 'mb'), 'tp'), parts along dimension 0
The draws below stay inside these ranges and needn't reach their ends.
There are 2 independent parts, one for each index of `grp`. The reference program is written for one: setup_inputs(seed, part) draws one part's arguments, and reference() takes and returns one part's arrays. A program takes and returns all parts, laid end to end along the dimension named above; an argument that names none is the same for every part. Nothing has to cross between parts.
Inputs may be any that keep to these rules, and one draw needn't show every extreme that they name: `expert_ids`: each row names 8 different experts; in every draw some expert is named by every token. slots[t, k] is the rank of the choice (t, k) among the choices of the same expert made by the 16 tokens of one device; these ranks are distinct and run from 0 upward. A choice whose slot is 8 or more is dropped.
All inputs are finite; a program needn't handle non-finite values.
Results may differ from the reference program's by a relative error of at most 0.017.
Values may be sent and summed in bfloat16 or wider, within the bound.
No kernel may reach another device: no remote copies, remote signals or barrier semaphores. Data moves between devices by JAX's collectives and lax.ppermute only.
A program may use at most 128 MiB of HBM per device.

```python
import math
import jax
import jax.numpy as jnp
from jax import lax

D = 3584
H = 1024
HEADS = 64
LAT = 512
KVC = 576
TOP = 8
TOK_DEV = 16
KV = 128
CAP = 8
EXPERTS = 32
TOKENS = 512
N_TP = 8


def routing(key):
    base_key = jax.random.fold_in(key, 7)
    hot_expert = jax.random.randint(jax.random.fold_in(base_key, 1), (), 0, EXPERTS)
    expert_iota = jnp.arange(EXPERTS, dtype=jnp.int32)
    biases = jax.random.randint(jax.random.fold_in(base_key, 2), (EXPERTS,), 0, 4 * EXPERTS)
    biases = jnp.where(expert_iota == hot_expert, 16 * EXPERTS, biases)
    noise_int = jax.random.randint(jax.random.fold_in(base_key, 3), (TOKENS, EXPERTS), 0, 6 * EXPERTS)
    scores = (noise_int + biases[None, :]) * EXPERTS + expert_iota[None, :]
    chosen = lax.top_k(scores, TOP)[1].astype(jnp.int32)
    priority = jax.random.randint(jax.random.fold_in(base_key, 4), (TOKENS, TOP), 0, 4096) * (TOKENS * TOP)
    priority = priority + jnp.arange(TOKENS * TOP, dtype=jnp.int32).reshape(TOKENS, TOP)
    blocks = TOKENS // TOK_DEV
    block_ids = chosen.reshape(blocks, TOK_DEV * TOP)
    block_prio = priority.reshape(blocks, TOK_DEV * TOP)
    same_expert = block_ids[:, :, None] == block_ids[:, None, :]
    earlier = block_prio[:, None, :] < block_prio[:, :, None]
    ranks = jnp.sum((same_expert & earlier).astype(jnp.int32), -1)
    return (chosen, ranks.reshape(TOKENS, TOP).astype(jnp.int32))


def draw_expert_ids(key, part):
    return routing(key)[0]


def draw_slots(key, part):
    return routing(key)[1]


def cache_normal(key):
    return jnp.clip(jax.random.normal(jax.random.fold_in(key, 31), (TOKENS, KV, KVC), jnp.float32), -4.0, 4.0)


def draw_cache(key, part):
    values = cache_normal(key)
    return values.astype(jnp.bfloat16)


def draw_queries(key, part):
    values = jnp.clip(jax.random.normal(jax.random.fold_in(key, 34), (TOKENS, HEADS, KVC), jnp.float32), -4.0, 4.0)
    return values.astype(jnp.bfloat16)


def draw_hidden(key, part):
    column_scale = 0.6 + 1.2 * jnp.arange(D, dtype=jnp.float32) / D
    values = jnp.clip(jax.random.normal(jax.random.fold_in(key, 44), (TOKENS, D), jnp.float32), -4.0, 4.0) * column_scale[None, :]
    return jnp.clip(values, -12.0, 12.0).astype(jnp.bfloat16)


def set_ends(result, rng, smallest, top_value):
    dims = result.shape
    place = [jax.random.randint(jax.random.fold_in(rng, axis), (), 0, dims[axis]) for axis in range(len(dims))]
    result = result.at[tuple(place)].set(smallest)
    longest = dims.index(max(dims))
    place[longest] = (place[longest] + 1) % dims[longest]
    return result.at[tuple(place)].set(top_value)


def block_levels(key, shape, cuts, smallest, largest):
    level = 1.0
    for dim, parts in cuts:
        draws = jax.random.uniform(jax.random.fold_in(jax.random.fold_in(key, 6), dim), (parts,), jnp.float32, smallest / len(cuts), largest / len(cuts))
        level = level * jnp.repeat(jnp.exp(draws), shape[dim] // parts).reshape((-1,) + (1,) * (len(shape) - 1 - dim))
    return level


def centred(own_key, dims, spread, limit, cuts=(), kind=jnp.bfloat16):
    loudness = block_levels(own_key, dims, cuts, -0.22, 0.18) if cuts else 1.0
    array = jax.random.normal(own_key, dims, jnp.float32) * spread * loudness
    return jnp.minimum(jnp.maximum(array, -limit), limit).astype(kind)


def setup_inputs(seed: int = 0, part: int = 0) -> dict:
    splits = jax.random.split(jax.random.key(seed), 15)
    part_keys = jax.random.split(jax.random.fold_in(splits[14], part), 15)
    hidden = draw_hidden(jax.random.fold_in(jax.random.fold_in(splits[14], part), 71), part)
    moe_gain = jnp.clip(1.0 + 0.18 * jax.random.normal(splits[1], (D,), jnp.float32), 0.1, 1.9)
    expert_ids = draw_expert_ids(jax.random.fold_in(jax.random.fold_in(splits[14], part), 71), part)
    slots = draw_slots(jax.random.fold_in(jax.random.fold_in(splits[14], part), 71), part)
    affinity = jnp.clip(jnp.exp(math.log(1.0) - 2.9957323 * jax.random.uniform(part_keys[4], (TOKENS, TOP), jnp.float32) ** block_levels(part_keys[4], (TOKENS, TOP), ((0, 32),), -0.2, 0.2)), 0.05, 1.0)
    w_gate = centred(splits[5], (EXPERTS, D, H), D ** -0.5, 0.09375, ((0, 32), (2, 8)))
    w_up = centred(splits[6], (EXPERTS, D, H), D ** -0.5, 0.09375, ((0, 32), (2, 8)))
    w_down = centred(splits[7], (EXPERTS, H, D), H ** -0.5, 0.1875, ((0, 32), (1, 8)))
    attn_gain = jnp.clip(1.0 + 0.18 * jax.random.normal(splits[8], (D,), jnp.float32), 0.1, 1.9)
    w_dkv = centred(splits[9], (D, KVC), D ** -0.5, 0.09375, ((0, 8),))
    kv_gain = jnp.clip(1.0 + 0.18 * jax.random.normal(splits[10], (LAT,), jnp.float32), 0.1, 1.9)
    queries = draw_queries(jax.random.fold_in(jax.random.fold_in(splits[14], part), 71), part)
    cache = draw_cache(jax.random.fold_in(jax.random.fold_in(splits[14], part), 71), part)
    lengths = set_ends(jax.random.randint(part_keys[13], (TOKENS,), 2, KV + 1), jax.random.fold_in(part_keys[13], 1), 2, KV).astype(jnp.int32)
    return dict(hidden=hidden, moe_gain=moe_gain, expert_ids=expert_ids, slots=slots, affinity=affinity, w_gate=w_gate, w_up=w_up, w_down=w_down, attn_gain=attn_gain, w_dkv=w_dkv, kv_gain=kv_gain, queries=queries, cache=cache, lengths=lengths)


epsilon = 1e-06
route_scale = 2.5
score_scale = 192.0 ** (-0.5)

def root_norm(values, gain):
    return values * lax.rsqrt(lax.optimization_barrier(jnp.mean(values * values, -1, keepdims=True)) + epsilon) * gain

def rope_rotate(rope_part, position):
    half_rope = rope_part.shape[-1] // 2
    inv_freq = 10000.0 ** (-jnp.arange(half_rope, dtype=jnp.float32) / half_rope)
    angles = position[:, None] * inv_freq[None, :]
    cos_table = jnp.cos(angles)
    sin_table = jnp.sin(angles)
    first_half = rope_part[:, :half_rope]
    second_half = rope_part[:, half_rope:]
    return jnp.concatenate([first_half * cos_table - second_half * sin_table, first_half * sin_table + second_half * cos_table], 1)

def reference(hidden, moe_gain, expert_ids, slots, affinity, w_gate, w_up, w_down, attn_gain, w_dkv, kv_gain, queries, cache, lengths):
    hidden_wide = hidden.astype(jnp.float32)
    normed = root_norm(hidden_wide, moe_gain).astype(jnp.bfloat16)
    kept_rows = slots < CAP
    weight = route_scale * affinity / lax.optimization_barrier(jnp.sum(affinity, -1, keepdims=True)) * kept_rows.astype(jnp.float32)
    source = (jnp.arange(TOKENS, dtype=jnp.int32) // TOK_DEV)[:, None]
    flat_slot = ((expert_ids * EXPERTS + source) * CAP + jnp.minimum(slots, CAP - 1)).astype(jnp.int32)
    slot_count = EXPERTS * EXPERTS * CAP
    token_iota = jnp.broadcast_to(jnp.arange(TOKENS, dtype=jnp.int32)[:, None], (TOKENS, TOP))
    target = jnp.where(kept_rows, flat_slot, slot_count).astype(jnp.int32)
    token_of = jnp.full((slot_count,), TOKENS, jnp.int32).at[target].set(token_iota, mode='drop')
    padded = jnp.concatenate([normed, jnp.zeros((1, D), jnp.bfloat16)], 0)
    expert_rows = padded[token_of].reshape(EXPERTS, EXPERTS * CAP, D)

    def expert_block(operands):
        rows_in, gate_weight, up_weight, down_weight = operands
        gate_act = jnp.dot(rows_in, gate_weight, preferred_element_type=jnp.float32)
        up_act = jnp.dot(rows_in, up_weight, preferred_element_type=jnp.float32)
        units = (jax.nn.silu(gate_act) * up_act).astype(jnp.bfloat16)
        grouped = units.reshape(EXPERTS * CAP, N_TP, H // N_TP).astype(jnp.float32)
        down_groups = down_weight.reshape(N_TP, H // N_TP, D).astype(jnp.float32)
        partials = jnp.einsum('rth,thd->trd', grouped, down_groups)
        return lax.optimization_barrier(jnp.sum(partials.astype(jnp.bfloat16).astype(jnp.float32), 0))
    expert_out = lax.map(expert_block, (expert_rows, w_gate, w_up, w_down)).reshape(slot_count, D)
    picked = expert_out[jnp.where(kept_rows, flat_slot, 0).astype(jnp.int32)]
    moe_out = lax.optimization_barrier(jnp.sum(picked * weight[:, :, None], 1))
    next_hidden = (hidden_wide + moe_out).astype(jnp.bfloat16)
    normed_attn = root_norm(next_hidden.astype(jnp.float32), attn_gain).astype(jnp.bfloat16)
    down_kv = jnp.dot(normed_attn, w_dkv, preferred_element_type=jnp.float32)
    latent_part = root_norm(down_kv[:, :LAT], kv_gain)
    rope_part = rope_rotate(down_kv[:, LAT:], lengths.astype(jnp.float32))
    new_key = jnp.concatenate([latent_part, rope_part], 1).astype(jnp.bfloat16)
    query_wide = queries.astype(jnp.float32)
    cache_wide = cache.astype(jnp.float32)
    scores = jnp.einsum('bhc,bjc->bhj', query_wide, cache_wide) * score_scale
    live_mask = (jnp.arange(KV, dtype=jnp.int32)[None, :] < lengths[:, None])[:, None, :]
    scores = jnp.where(live_mask, scores, -1e+30)
    own_score = jnp.einsum('bhc,bc->bh', query_wide, new_key.astype(jnp.float32)) * score_scale
    peak_all = jnp.maximum(lax.optimization_barrier(jnp.max(scores, -1)), own_score)
    prob_live = jnp.where(live_mask, jnp.exp(scores - peak_all[:, :, None]), 0.0)
    own_prob = jnp.exp(own_score - peak_all)
    mass_total = lax.optimization_barrier(jnp.sum(prob_live, -1)) + own_prob
    numerator = jnp.einsum('bhj,bjc->bhc', prob_live.astype(jnp.bfloat16).astype(jnp.float32), cache_wide[:, :, :LAT])
    numerator = numerator + own_prob.astype(jnp.bfloat16).astype(jnp.float32)[:, :, None] * new_key[:, None, :LAT].astype(jnp.float32)
    latent_out = (numerator / mass_total[:, :, None]).astype(jnp.bfloat16)
    return (next_hidden, latent_out)
```

```python
import jax
import jax.numpy as jnp
from jax import lax
from jax.experimental import pallas as pl
from jax.experimental.pallas import tpu as pltpu
from jax.sharding import PartitionSpec as P

D = 3584
LAT = 512
CAP = 8
EXTRA = 8

epsilon = 1e-06
route_scale = 2.5
score_scale = 192.0 ** (-0.5)
f32 = jnp.float32
bf16 = jnp.bfloat16


def parts_of(x):
    hi = lax.reduce_precision(x, 8, 7)
    mid = lax.reduce_precision(x - hi, 8, 7)
    lo = x - hi - mid
    return hi.astype(bf16), mid.astype(bf16), lo.astype(bf16)


def rope_rotate(rope_part, position):
    half_rope = rope_part.shape[-1] // 2
    inv_freq = 10000.0 ** (-jnp.arange(half_rope, dtype=f32) / half_rope)
    angles = position[:, None] * inv_freq[None, :]
    cos_table = jnp.cos(angles)
    sin_table = jnp.sin(angles)
    first_half = rope_part[:, :half_rope]
    second_half = rope_part[:, half_rope:]
    return jnp.concatenate(
        [
            first_half * cos_table - second_half * sin_table,
            first_half * sin_table + second_half * cos_table,
        ],
        1,
    )


def expert_kernel(x_ref, wg_ref, wu_ref, wd_ref, o_ref, g_ref, u_ref):
    peers, padded, cols = x_ref.shape
    rows = padded - EXTRA
    square = jnp.zeros((rows, 1), f32)
    for j in range(peers):
        x = x_ref[j, :rows, :].astype(f32)
        square = square + jnp.sum(x * x, -1, keepdims=True)
    scale = lax.rsqrt(square / D + epsilon)
    for j in range(peers):
        x = x_ref[j, :rows, :].astype(f32)
        gain = jnp.sum(x_ref[j, rows:, :].astype(f32), 0, keepdims=True)
        normed = (x * scale * gain).astype(bf16)
        part = pl.ds(j * cols, cols)
        gate = jnp.dot(normed, wg_ref[part, :], preferred_element_type=f32)
        up = jnp.dot(normed, wu_ref[part, :], preferred_element_type=f32)
        if j == 0:
            g_ref[...] = gate
            u_ref[...] = up
        else:
            g_ref[...] += gate
            u_ref[...] += up
    gate = g_ref[...]
    units = (gate / (1.0 + jnp.exp(-gate)) * u_ref[...]).astype(bf16)
    for j in range(peers):
        o_ref[j] = jnp.dot(
            units, wd_ref[:, j * cols : (j + 1) * cols], preferred_element_type=f32
        ).astype(bf16)


def expert(x, w_gate, w_up, w_down):
    peers, padded, cols = x.shape
    rows = padded - EXTRA
    hid = w_gate.shape[1]
    vmem = pl.BlockSpec(memory_space=pltpu.VMEM)
    return pl.pallas_call(
        expert_kernel,
        out_shape=jax.ShapeDtypeStruct((peers, rows, cols), bf16),
        in_specs=[vmem] * 4,
        out_specs=vmem,
        scratch_shapes=[pltpu.VMEM((rows, hid), f32), pltpu.VMEM((rows, hid), f32)],
        compiler_params=pltpu.CompilerParams(vmem_limit_bytes=40 * 1024 * 1024),
        name="expert",
    )(x, w_gate, w_up, w_down)


def cached_attention(queries, cache, lengths):
    seqs, heads, keys = queries.shape
    peers = lax.axis_size("tp")
    own = seqs // peers
    span = cache.shape[1]
    both = jnp.concatenate([cache, queries], 1)
    moved = lax.all_to_all(
        both.reshape(peers, own, span + heads, keys), "tp", split_axis=0, concat_axis=0, tiled=True
    )
    full_cache = jnp.moveaxis(moved[:, :, :span], 0, 1).reshape(own, peers * span, keys)
    full_queries = jnp.moveaxis(moved[:, :, span:], 0, 1).reshape(own, peers * heads, keys)
    live_of = lax.dynamic_slice(lengths, (lax.axis_index("tp") * own,), (own,))
    position = jnp.arange(peers * span, dtype=jnp.int32)
    live = (position[None, :] < live_of[:, None])[:, None, :]
    scores = (
        jnp.einsum("bhc,bjc->bhj", full_queries, full_cache, preferred_element_type=f32)
        * score_scale
    )
    scores = jnp.where(live, scores, -1e30)
    peak = jnp.max(scores, -1)
    prob = jnp.where(live, jnp.exp(scores - peak[:, :, None]), 0.0)
    mass = jnp.sum(prob, -1)
    out = jnp.einsum(
        "bhj,bjc->bhc", prob.astype(bf16), full_cache[:, :, :LAT], preferred_element_type=f32
    )
    out = (out / mass[:, :, None]).astype(bf16)
    log_mass = peak + jnp.log(mass)
    tail = jnp.stack(parts_of(log_mass), -1)
    tail = jnp.pad(tail, ((0, 0), (0, 0), (0, 125)))
    back = jnp.concatenate([out, tail], -1).reshape(own, peers, heads, LAT + 128)
    back = lax.all_to_all(
        jnp.moveaxis(back, 1, 0), "tp", split_axis=0, concat_axis=0, tiled=True
    ).reshape(seqs, heads, LAT + 128)
    return back[:, :, :LAT].astype(f32), jnp.sum(back[:, :, LAT : LAT + 3].astype(f32), -1)


def local(
    hidden,
    moe_gain,
    expert_ids,
    slots,
    affinity,
    w_gate,
    w_up,
    w_down,
    attn_gain,
    w_dkv,
    kv_gain,
    queries,
    cache,
    lengths,
):
    tok_rows, width = hidden.shape
    experts = lax.axis_size("ep") * lax.axis_size("mb")
    slot_rows = experts * CAP
    hidden_wide = hidden.astype(f32)
    kept_rows = slots < CAP
    weight = (
        route_scale
        * affinity
        / jnp.sum(affinity, -1, keepdims=True)
        * kept_rows.astype(f32)
    )
    target = jnp.where(kept_rows, expert_ids * CAP + slots, -1)
    matches = target[None, :, :] == jnp.arange(slot_rows, dtype=jnp.int32)[:, None, None]
    dispatch = jnp.any(matches, 2).astype(bf16)
    combine = jnp.sum(jnp.where(matches, weight[None, :, :], 0.0), 2).T
    send_rows = jnp.dot(dispatch, hidden, preferred_element_type=f32).astype(bf16)
    arrived = lax.all_to_all(
        send_rows.reshape(experts, CAP, width),
        ("ep", "mb"),
        split_axis=0,
        concat_axis=0,
        tiled=True,
    ).reshape(slot_rows, width)
    gain_rows = jnp.pad(jnp.stack(parts_of(moe_gain)), ((0, EXTRA - 3), (0, 0)))
    portion = lax.all_gather(jnp.concatenate([arrived, gain_rows], 0), "tp")
    partial_out = expert(portion, w_gate[0], w_up[0], w_down[0])
    summed = lax.psum_scatter(partial_out, "tp")
    returned = lax.all_to_all(
        summed.reshape(experts, CAP, width),
        ("ep", "mb"),
        split_axis=0,
        concat_axis=0,
        tiled=True,
    ).reshape(slot_rows, width)
    moe_out = jnp.dot(combine, returned)
    next_hidden = (hidden_wide + moe_out).astype(bf16)
    next_wide = next_hidden.astype(f32)

    cached_out, cached_mass = cached_attention(queries, cache, lengths)

    keys = w_dkv.shape[1]
    down = jnp.dot(
        (next_wide * attn_gain).astype(bf16), w_dkv, preferred_element_type=f32
    )
    square = jnp.sum(next_wide * next_wide, -1, keepdims=True)
    small = jnp.concatenate([down, jnp.broadcast_to(square, (tok_rows, 64))], 1)
    peers = lax.axis_size("tp")
    shared = jnp.sum(
        lax.all_to_all(
            jnp.broadcast_to(small, (peers, *small.shape)),
            "tp",
            split_axis=0,
            concat_axis=0,
            tiled=True,
        ),
        0,
    )
    down_kv = shared[:, :keys] * lax.rsqrt(shared[:, keys : keys + 1] / D + epsilon)
    latent_part = down_kv[:, :LAT]
    latent_part = (
        latent_part
        * lax.rsqrt(jnp.mean(latent_part * latent_part, -1, keepdims=True) + epsilon)
        * kv_gain
    )
    rope_part = rope_rotate(down_kv[:, LAT:], lengths.astype(f32))
    new_key = jnp.concatenate([latent_part, rope_part], 1).astype(bf16)
    own_score = (
        jnp.einsum("bhc,bc->bh", queries, new_key, preferred_element_type=f32) * score_scale
    )
    peak_all = jnp.maximum(own_score, cached_mass)
    own_prob = jnp.exp(own_score - peak_all)
    cached_prob = jnp.exp(cached_mass - peak_all)
    share = 1.0 / (own_prob + cached_prob)
    latent_out = (
        cached_out * (cached_prob * share)[:, :, None]
        + new_key[:, None, :LAT].astype(f32) * (own_prob * share)[:, :, None]
    ).astype(bf16)
    return (next_hidden, latent_out)


def solution(mesh):
    return jax.shard_map(
        local,
        mesh=mesh,
        in_specs=(
            P(("grp", "ep", "mb"), "tp"),
            P("tp"),
            P(("grp", "ep", "mb"), None),
            P(("grp", "ep", "mb"), None),
            P(("grp", "ep", "mb"), None),
            P(("ep", "mb"), None, "tp"),
            P(("ep", "mb"), None, "tp"),
            P(("ep", "mb"), "tp", None),
            P("tp"),
            P("tp", None),
            P(),
            P(("grp", "ep", "mb"), "tp", None),
            P(("grp", "ep", "mb"), "tp", None),
            P(("grp", "ep", "mb")),
        ),
        out_specs=(P(("grp", "ep", "mb"), "tp"), P(("grp", "ep", "mb"), "tp", None)),
        check_vma=False,
    )
```

```python
import jax
import jax.numpy as jnp
from jax import lax
from jax.experimental import pallas as pl
from jax.experimental.pallas import tpu as pltpu
from jax.sharding import PartitionSpec as P


D = 3584
LAT = 512
CAP = 8
EXTRA = 8

epsilon = 1e-06
route_scale = 2.5
score_scale = 192.0 ** (-0.5)
f32 = jnp.float32
bf16 = jnp.bfloat16
VMEM = pl.BlockSpec(memory_space=pltpu.VMEM)
SMEM = pl.BlockSpec(memory_space=pltpu.SMEM)
PARAMS = pltpu.CompilerParams(vmem_limit_bytes=40 * 1024 * 1024)


def shape(dims, dtype):
    return jax.ShapeDtypeStruct(dims, dtype)


def exchange(x, axis):
    return lax.all_to_all(x, axis, split_axis=0, concat_axis=0, tiled=True)


def route_kernel(ids_ref, slots_ref, aff_ref, hid_ref, send_ref, comb_ref):
    experts = send_ref.shape[0]
    tokens, top = ids_ref.shape
    rows = experts * CAP
    slots = slots_ref[...]
    kept = slots < CAP
    affinity = aff_ref[...]
    weight = route_scale * affinity / jnp.sum(affinity, -1, keepdims=True)
    target = jnp.where(kept, ids_ref[...] * CAP + slots, -1)
    lane = lax.broadcasted_iota(jnp.int32, (tokens, rows), 1)
    pick = jnp.zeros((tokens, rows), f32)
    comb = jnp.zeros((tokens, rows), f32)
    for k in range(top):
        match = target[:, k : k + 1] == lane
        pick = jnp.where(match, 1.0, pick)
        comb = jnp.where(match, weight[:, k : k + 1], comb)
    comb_ref[...] = comb
    sent = lax.dot_general(
        pick.astype(bf16), hid_ref[...], (((0,), (0,)), ((), ())), preferred_element_type=f32
    )
    send_ref[...] = sent.reshape(send_ref.shape).astype(bf16)


def route(expert_ids, slots, affinity, hidden, experts):
    tokens, width = hidden.shape
    return pl.pallas_call(
        route_kernel,
        out_shape=(shape((experts, CAP, width), bf16), shape((tokens, experts * CAP), f32)),
        in_specs=[VMEM] * 4,
        out_specs=(VMEM, VMEM),
        compiler_params=PARAMS,
        name="route",
    )(expert_ids, slots, affinity, hidden)


def units_kernel(x_ref, wg_ref, wu_ref, o_ref, g_ref, u_ref):
    peers, padded, cols = x_ref.shape
    rows = padded - EXTRA
    square = jnp.zeros((rows, 1), f32)
    for j in range(peers):
        x = x_ref[j, :rows, :].astype(f32)
        square = square + jnp.sum(x * x, -1, keepdims=True)
    scale = lax.rsqrt(square / D + epsilon)
    for j in range(peers):
        x = x_ref[j, :rows, :].astype(f32)
        gain = jnp.sum(x_ref[j, rows:, :].astype(f32), 0, keepdims=True)
        normed = (x * scale * gain).astype(bf16)
        part = pl.ds(j * cols, cols)
        gate = jnp.dot(normed, wg_ref[part, :], preferred_element_type=f32)
        up = jnp.dot(normed, wu_ref[part, :], preferred_element_type=f32)
        if j == 0:
            g_ref[...] = gate
            u_ref[...] = up
        else:
            g_ref[...] += gate
            u_ref[...] += up
    gate = g_ref[...]
    units = (gate / (1.0 + jnp.exp(-gate)) * u_ref[...]).astype(bf16)
    for j in range(peers):
        o_ref[j] = units


def expert_units(x, w_gate, w_up):
    peers, padded, _ = x.shape
    rows, hid = padded - EXTRA, w_gate.shape[1]
    return pl.pallas_call(
        units_kernel,
        out_shape=shape((peers, rows, hid), bf16),
        in_specs=[VMEM] * 3,
        out_specs=VMEM,
        scratch_shapes=[pltpu.VMEM((rows, hid), f32), pltpu.VMEM((rows, hid), f32)],
        compiler_params=PARAMS,
        name="units",
    )(x, w_gate, w_up)


def pack_kernel(me_ref, wd_ref, cache_ref, q_ref, *refs):
    outs, tiles_ref = refs[:-1], refs[-1]
    peers = len(outs)
    hid, width = tiles_ref.shape[1:]
    span, heads, keys = cache_ref.shape[1], q_ref.shape[1], cache_ref.shape[2]
    own = cache_ref.shape[0] // peers
    for j in range(peers):
        tiles_ref[j] = wd_ref[:, j * width : (j + 1) * width]
    for k in range(peers):
        to = lax.rem(me_ref[0] + k, peers)
        outs[k][:hid, :width] = tiles_ref[to]
        outs[k][:hid, width:] = jnp.zeros((hid, keys - width), bf16)
        for i in range(own):
            row = hid + i * (span + heads)
            outs[k][row : row + span, :] = cache_ref[to * own + i]
            outs[k][row + span : row + span + heads, :] = q_ref[to * own + i]


def pack(me, w_down, cache, queries, peers):
    hid, width = w_down.shape[0], w_down.shape[1] // peers
    seqs, span, keys = cache.shape
    rows = hid + seqs // peers * (span + queries.shape[1])
    return pl.pallas_call(
        pack_kernel,
        out_shape=tuple(shape((rows, keys), bf16) for _ in range(peers)),
        in_specs=[SMEM] + [VMEM] * 3,
        out_specs=tuple(VMEM for _ in range(peers)),
        scratch_shapes=[pltpu.VMEM((peers, hid, width), bf16)],
        compiler_params=PARAMS,
        name="pack",
    )(me, w_down, cache, queries)


def spread_kernel(x_ref, gain_ref, o_ref):
    rows = o_ref.shape[1] - EXTRA
    gain = gain_ref[...]
    first = gain.astype(bf16).astype(f32)
    second = (gain - first).astype(bf16).astype(f32)
    third = gain - first - second
    row = lax.broadcasted_iota(jnp.int32, (EXTRA, gain.shape[1]), 0)
    tail = jnp.where(
        row == 0, first, jnp.where(row == 1, second, jnp.where(row == 2, third, 0.0))
    ).astype(bf16)
    x = x_ref[...].reshape(rows, gain.shape[1])
    for j in range(o_ref.shape[0]):
        o_ref[j, :rows, :] = x
        o_ref[j, rows:, :] = tail


def spread_rows(arrived, gain, peers):
    experts, cap, width = arrived.shape
    return pl.pallas_call(
        spread_kernel,
        out_shape=shape((peers, experts * cap + EXTRA, width), bf16),
        in_specs=[VMEM] * 2,
        out_specs=VMEM,
        compiler_params=PARAMS,
        name="rows",
    )(arrived, gain)


def down_kernel(me_ref, u_ref, *refs):
    blocks, o_ref = refs[:-1], refs[-1]
    peers, _, hid = u_ref.shape
    width = o_ref.shape[-1]
    acc = jnp.zeros((u_ref.shape[1], width), f32)
    for k in range(peers):
        group = lax.rem(me_ref[0] + (peers - k), peers)
        acc = acc + jnp.dot(
            u_ref[group], blocks[k][:hid, :width], preferred_element_type=f32
        )
    o_ref[...] = acc.reshape(o_ref.shape).astype(bf16)


def expert_down(me, units, blocks, experts, width):
    return pl.pallas_call(
        down_kernel,
        out_shape=shape((experts, CAP, width), bf16),
        in_specs=[SMEM] + [VMEM] * (1 + len(blocks)),
        out_specs=VMEM,
        compiler_params=PARAMS,
        name="down",
    )(me, units, *blocks)


def attend_kernel(me_ref, len_ref, *refs):
    peers = (len(refs) - 2) // 2
    blocks, outs, c_ref, q_ref = refs[:peers], refs[peers:-2], refs[-2], refs[-1]
    own, heads, _ = outs[0].shape
    span = c_ref.shape[1] // peers
    first = blocks[0].shape[0] - own * (span + heads)
    me = me_ref[0]
    for i in range(own):
        for k in range(peers):
            row = first + i * (span + heads)
            c_ref[i, k * span : (k + 1) * span, :] = blocks[k][row : row + span, :]
            q_ref[i, k * heads : (k + 1) * heads, :] = blocks[k][
                row + span : row + span + heads, :
            ]
    lane = lax.broadcasted_iota(jnp.int32, (peers * heads, peers * span), 1)
    block = lax.rem(me + (peers - lane // span), peers)
    position = block * span + lane % span
    for i in range(own):
        live = position < len_ref[me * own + i]
        keys = c_ref[i]
        scores = (
            lax.dot_general(
                q_ref[i], keys, (((1,), (1,)), ((), ())), preferred_element_type=f32
            )
            * score_scale
        )
        scores = jnp.where(live, scores, -1e30)
        peak = jnp.max(scores, -1, keepdims=True)
        prob = jnp.where(live, jnp.exp(scores - peak), 0.0)
        mass = jnp.sum(prob, -1, keepdims=True)
        out = jnp.dot(prob.astype(bf16), keys[:, :LAT], preferred_element_type=f32)
        out = (out / mass).astype(bf16)
        total = peak + jnp.log(mass)
        high = total.astype(bf16).astype(f32)
        middle = (total - high).astype(bf16).astype(f32)
        low = total - high - middle
        tail_lane = lax.broadcasted_iota(jnp.int32, (peers * heads, 128), 1)
        tail = jnp.where(
            tail_lane == 0,
            high,
            jnp.where(tail_lane == 1, middle, jnp.where(tail_lane == 2, low, 0.0)),
        ).astype(bf16)
        for k in range(peers):
            outs[k][i, :, :LAT] = out[k * heads : (k + 1) * heads]
            outs[k][i, :, LAT:] = tail[k * heads : (k + 1) * heads]


def attend(me, lengths, blocks, own, span, heads):
    peers, keys = len(blocks), blocks[0].shape[1]
    return pl.pallas_call(
        attend_kernel,
        out_shape=tuple(shape((own, heads, LAT + 128), bf16) for _ in range(peers)),
        in_specs=[SMEM, SMEM] + [VMEM] * peers,
        out_specs=tuple(VMEM for _ in range(peers)),
        scratch_shapes=[
            pltpu.VMEM((own, peers * span, keys), bf16),
            pltpu.VMEM((own, peers * heads, keys), bf16),
        ],
        compiler_params=PARAMS,
        name="attend",
    )(me, lengths, *blocks)


def close_kernel(ret_ref, comb_ref, hid_ref, gain_ref, wdkv_ref, next_ref, small_ref):
    rows = comb_ref.shape[1]
    keys = wdkv_ref.shape[1]
    returned = ret_ref[...].reshape(rows, ret_ref.shape[-1])
    comb = comb_ref[...]
    high = comb.astype(bf16)
    low = (comb - high.astype(f32)).astype(bf16)
    moe = jnp.dot(high, returned, preferred_element_type=f32) + jnp.dot(
        low, returned, preferred_element_type=f32
    )
    result = (hid_ref[...].astype(f32) + moe).astype(bf16)
    next_ref[...] = result
    wide = result.astype(f32)
    square = jnp.sum(wide * wide, -1, keepdims=True)
    first = square.astype(bf16).astype(f32)
    second = (square - first).astype(bf16).astype(f32)
    third = square - first - second
    lane = lax.broadcasted_iota(jnp.int32, (wide.shape[0], small_ref.shape[2] - keys), 1)
    tail = jnp.where(
        lane == 0, first, jnp.where(lane == 1, second, jnp.where(lane == 2, third, 0.0))
    ).astype(bf16)
    down = jnp.dot(
        (wide * gain_ref[...]).astype(bf16), wdkv_ref[...], preferred_element_type=f32
    ).astype(bf16)
    for j in range(small_ref.shape[0]):
        small_ref[j, :, :keys] = down
        small_ref[j, :, keys:] = tail


def close(returned, combine, hidden, gain, w_dkv, peers):
    tokens, width = hidden.shape
    return pl.pallas_call(
        close_kernel,
        out_shape=(
            shape((tokens, width), bf16),
            shape((peers, tokens, w_dkv.shape[1] + 64), bf16),
        ),
        in_specs=[VMEM] * 5,
        out_specs=(VMEM, VMEM),
        compiler_params=PARAMS,
        name="close",
    )(returned, combine, hidden, gain, w_dkv)


def merge_kernel(me_ref, all_ref, gain_ref, cos_ref, sin_ref, q_ref, *refs):
    backs, o_ref, back_ref = refs[:-2], refs[-2], refs[-1]
    peers = len(backs)
    own_seqs = backs[0].shape[0]
    for k in range(peers):
        source = lax.rem(me_ref[0] + k, peers)
        back_ref[pl.ds(source * own_seqs, own_seqs)] = backs[k][...]
    keys = q_ref.shape[-1]
    total = all_ref[0].astype(f32)
    for j in range(1, all_ref.shape[0]):
        total = total + all_ref[j].astype(f32)
    square = jnp.sum(total[:, keys:], -1, keepdims=True)
    down = total[:, :keys] * lax.rsqrt(square / D + epsilon)
    latent = down[:, :LAT]
    latent = (
        latent
        * lax.rsqrt(jnp.mean(latent * latent, -1, keepdims=True) + epsilon)
        * gain_ref[...]
    )
    rope = down[:, LAT:]
    half = rope.shape[-1] // 2
    turned = jnp.concatenate([rope[:, half:], rope[:, :half]], 1)
    rope = rope * cos_ref[...] + turned * sin_ref[...]
    latent = latent.astype(bf16).astype(f32)[:, None, :]
    rope = rope.astype(bf16).astype(f32)[:, None, :]
    own = (
        jnp.sum(q_ref[:, :, :LAT].astype(f32) * latent, -1, keepdims=True)
        + jnp.sum(q_ref[:, :, LAT:].astype(f32) * rope, -1, keepdims=True)
    ) * score_scale
    cached = jnp.sum(back_ref[:, :, LAT:].astype(f32), -1, keepdims=True)
    peak = jnp.maximum(own, cached)
    own_prob = jnp.exp(own - peak)
    cached_prob = jnp.exp(cached - peak)
    total_prob = own_prob + cached_prob
    o_ref[...] = (
        back_ref[:, :, :LAT].astype(f32) * (cached_prob / total_prob)
        + latent * (own_prob / total_prob)
    ).astype(bf16)


def merge(me, everything, gain, cos, sin, queries, backs):
    seqs, heads, _ = queries.shape
    return pl.pallas_call(
        merge_kernel,
        out_shape=shape((seqs, heads, LAT), bf16),
        in_specs=[SMEM] + [VMEM] * (5 + len(backs)),
        out_specs=VMEM,
        scratch_shapes=[pltpu.VMEM((seqs, heads, LAT + 128), bf16)],
        compiler_params=PARAMS,
        name="merge",
    )(me, everything, gain, cos, sin, queries, *backs)


def mark_kernel(x_ref, o_ref):
    o_ref[...] = x_ref[...]


def mark(x):
    return pl.pallas_call(
        mark_kernel, out_shape=shape(x.shape, x.dtype), in_specs=[VMEM], out_specs=VMEM
    )(x)


def rope_tables(lengths, half):
    inv_freq = 10000.0 ** (-jnp.arange(half, dtype=f32) / half)
    angles = lengths.astype(f32)[:, None] * inv_freq[None, :]
    cos, sin = jnp.cos(angles), jnp.sin(angles)
    return jnp.concatenate([cos, cos], 1), jnp.concatenate([-sin, sin], 1)


def local(
    hidden,
    moe_gain,
    expert_ids,
    slots,
    affinity,
    w_gate,
    w_up,
    w_down,
    attn_gain,
    w_dkv,
    kv_gain,
    queries,
    cache,
    lengths,
):
    seqs, width = hidden.shape
    peers = lax.axis_size("tp")
    experts = lax.axis_size("ep") * lax.axis_size("mb")
    me = lax.axis_index("tp").astype(jnp.int32).reshape(1)

    def moved(x, k):
        return lax.ppermute(x, "tp", [(i, (i + k) % peers) for i in range(peers)])

    send_rows, combine = route(expert_ids, slots, affinity, hidden, experts)
    arrived = exchange(send_rows, ("ep", "mb"))
    blocks = list(pack(me, w_down[0], cache, queries, peers))
    for k in range(1, peers):
        blocks[k] = moved(blocks[k], k)
    rows = spread_rows(arrived, mark(moe_gain[None]), peers)
    portion = exchange(rows, "tp")
    backs = list(attend(me, lengths, blocks, seqs // peers, cache.shape[1], queries.shape[1]))
    for k in range(1, peers):
        backs[k] = moved(backs[k], peers - k)
    units = expert_units(portion, w_gate[0], w_up[0])
    all_units = exchange(units, "tp")
    output = expert_down(me, all_units, blocks, experts, width)
    returned = exchange(output, ("ep", "mb"))
    attn_gain = mark(attn_gain[None])
    next_hidden, small = close(returned, combine, hidden, attn_gain, w_dkv, peers)
    everything = exchange(small, "tp")
    cos, sin = rope_tables(lengths, (queries.shape[-1] - LAT) // 2)
    latent_out = merge(me, everything, kv_gain[None], cos, sin, queries, backs)
    return (next_hidden, latent_out)


def solution(mesh):
    return jax.shard_map(
        local,
        mesh=mesh,
        in_specs=(
            P(("grp", "ep", "mb"), "tp"),
            P("tp"),
            P(("grp", "ep", "mb"), None),
            P(("grp", "ep", "mb"), None),
            P(("grp", "ep", "mb"), None),
            P(("ep", "mb"), None, "tp"),
            P(("ep", "mb"), None, "tp"),
            P(("ep", "mb"), "tp", None),
            P("tp"),
            P("tp", None),
            P(),
            P(("grp", "ep", "mb"), "tp", None),
            P(("grp", "ep", "mb"), "tp", None),
            P(("grp", "ep", "mb")),
        ),
        out_specs=(P(("grp", "ep", "mb"), "tp"), P(("grp", "ep", "mb"), "tp", None)),
        check_vma=False,
    )
```

```python
import jax
import jax.numpy as jnp
from jax import lax
from jax.experimental import pallas as pl
from jax.experimental.pallas import tpu as pltpu
from jax.sharding import PartitionSpec as P


D = 3584
LAT = 512
CAP = 8
MOVES = (4, 3, 5, 2, 6, 1, 7)

epsilon = 1e-06
route_scale = 2.5
score_scale = 192.0 ** (-0.5)
f32 = jnp.float32
bf16 = jnp.bfloat16
VMEM = pl.BlockSpec(memory_space=pltpu.VMEM)
SMEM = pl.BlockSpec(memory_space=pltpu.SMEM)
PARAMS = pltpu.CompilerParams(vmem_limit_bytes=40 * 1024 * 1024)


def shape(dims, dtype):
    return jax.ShapeDtypeStruct(dims, dtype)


def exchange(x, axis):
    return lax.all_to_all(x, axis, split_axis=0, concat_axis=0, tiled=True)


def route_kernel(ids_ref, slots_ref, aff_ref, hid_ref, send_ref, comb_ref):
    experts = send_ref.shape[0]
    top, tokens = ids_ref.shape
    rows = experts * CAP
    slots = slots_ref[...]
    affinity = aff_ref[...]
    weight = route_scale * affinity / jnp.sum(affinity, 0, keepdims=True)
    target = jnp.where(slots < CAP, ids_ref[...] * CAP + slots, -1)
    row = lax.broadcasted_iota(jnp.int32, (rows, tokens), 0)
    pick = jnp.zeros((rows, tokens), f32)
    comb = jnp.zeros((rows, tokens), f32)
    for k in range(top):
        match = target[k : k + 1, :] == row
        pick = jnp.where(match, 1.0, pick)
        comb = jnp.where(match, weight[k : k + 1, :], comb)
    comb_ref[...] = comb
    sent = jnp.dot(pick.astype(bf16), hid_ref[...], preferred_element_type=f32)
    send_ref[...] = sent.reshape(send_ref.shape).astype(bf16)


def route(expert_ids, slots, affinity, hidden, experts):
    tokens, width = hidden.shape
    return pl.pallas_call(
        route_kernel,
        out_shape=(shape((experts, CAP, width), bf16), shape((experts * CAP, tokens), f32)),
        in_specs=[VMEM] * 4,
        out_specs=(VMEM, VMEM),
        compiler_params=PARAMS,
        name="route",
    )(expert_ids.T, slots.T, affinity.T, hidden)


def gain_of(block, at, width):
    rows = block[at : at + 16, :].astype(f32)
    tiles = (width + 127) // 128
    total = rows[:tiles] + rows[tiles : 2 * tiles] + rows[2 * tiles : 3 * tiles]
    return [total[q : q + 1, : min(128, width - 128 * q)] for q in range(tiles)]


def units_kernel(me_ref, x_ref, wg_ref, wu_ref, att_ref, *refs):
    peers = x_ref.shape[0]
    blocks, (o_ref, n_ref, g_ref, u_ref) = refs[:peers], refs[peers:]
    half, double = x_ref.shape[1:]
    rows, cols = 2 * half, double // 2
    square = jnp.zeros((rows, 1), f32)
    for j in range(peers):
        n_ref[:half, :] = x_ref[j, :, :cols]
        n_ref[half:, :] = x_ref[j, :, cols:]
        x = n_ref[...].astype(f32)
        square = square + jnp.sum(x * x, -1, keepdims=True)
    scale = lax.rsqrt(square / D + epsilon)
    for k in range(peers):
        j = lax.rem(me_ref[0] + (peers - k), peers)
        gain = jnp.concatenate(gain_of(blocks[k], blocks[k].shape[0] - 16, cols), 1)
        n_ref[:half, :] = x_ref[j, :, :cols]
        n_ref[half:, :] = x_ref[j, :, cols:]
        normed = (n_ref[...].astype(f32) * scale * gain).astype(bf16)
        part = pl.ds(pl.multiple_of(j * cols, 64), cols)
        gate = jnp.dot(normed, wg_ref[part, :], preferred_element_type=f32)
        up = jnp.dot(normed, wu_ref[part, :], preferred_element_type=f32)
        if k == 0:
            g_ref[...] = gate
            u_ref[...] = up
        else:
            g_ref[...] += gate
            u_ref[...] += up
        o_ref[j, rows:, :] = att_ref[k]
    gate = g_ref[...]
    units = (gate / (1.0 + jnp.exp(-gate)) * u_ref[...]).astype(bf16)
    for j in range(peers):
        o_ref[j, :rows, :] = units


def expert_units(me, x, w_gate, w_up, attended, blocks):
    peers, half, double = x.shape
    rows, cols, hid = 2 * half, double // 2, w_gate.shape[1]
    return pl.pallas_call(
        units_kernel,
        out_shape=shape((peers, rows + attended.shape[1], hid), bf16),
        in_specs=[SMEM] + [VMEM] * (4 + peers),
        out_specs=VMEM,
        scratch_shapes=[
            pltpu.VMEM((rows, cols), bf16),
            pltpu.VMEM((rows, hid), f32),
            pltpu.VMEM((rows, hid), f32),
        ],
        compiler_params=PARAMS,
        name="units",
    )(me, x, w_gate, w_up, attended, *blocks)


def pack_kernel(me_ref, wd_ref, cache_ref, q_ref, gain_ref, *refs):
    outs, tiles_ref, keys_ref = refs[:-2], refs[-2], refs[-1]
    peers = len(outs)
    half, double = tiles_ref.shape[1:]
    width = double // 2
    span, heads, keys = cache_ref.shape[1], q_ref.shape[1], cache_ref.shape[2]
    own = cache_ref.shape[0] // peers
    for j in range(peers):
        tiles_ref[j, :, :width] = wd_ref[:half, j * width : (j + 1) * width]
        tiles_ref[j, :, width:] = wd_ref[half:, j * width : (j + 1) * width]
    gain = gain_ref[...]
    first = gain.astype(bf16).astype(f32)
    second = (gain - first).astype(bf16).astype(f32)
    row = lax.broadcasted_iota(jnp.int32, (16, 128), 0)
    packed = jnp.zeros((16, 128), f32)
    tiles = (width + 127) // 128
    for p, value in enumerate((first, second, gain - first - second)):
        for q in range(tiles):
            piece = value[:, 128 * q : min(128 * (q + 1), width)]
            if piece.shape[1] < 128:
                piece = jnp.concatenate([piece, jnp.zeros((1, 128 - piece.shape[1]), f32)], 1)
            packed = jnp.where(row == p * tiles + q, piece, packed)
    packed = packed.astype(bf16)
    for k in range(peers):
        to = lax.rem(me_ref[0] + k, peers)
        at = 0
        for t in range(double // 128):
            outs[k][at : at + half, :] = tiles_ref[to, :, 128 * t : 128 * (t + 1)]
            at += half
        for i in range(own):
            keys_ref[:span, i * keys : (i + 1) * keys] = cache_ref[to * own + i]
            keys_ref[span:, i * keys : (i + 1) * keys] = q_ref[to * own + i]
        for t in range(own * keys // 128):
            outs[k][at : at + span + heads, :] = keys_ref[:, 128 * t : 128 * (t + 1)]
            at += span + heads
        outs[k][at : at + 16, :] = packed


def pack(me, w_down, cache, queries, gain, peers):
    hid, width = w_down.shape[0], w_down.shape[1] // peers
    seqs, span, keys = cache.shape
    own, heads = seqs // peers, queries.shape[1]
    rows = hid * width // 128 + own * (span + heads) * keys // 128 + 16
    return pl.pallas_call(
        pack_kernel,
        out_shape=tuple(shape((rows, 128), bf16) for _ in range(peers)),
        in_specs=[SMEM] + [VMEM] * 4,
        out_specs=tuple(VMEM for _ in range(peers)),
        scratch_shapes=[
            pltpu.VMEM((peers, hid // 2, 2 * width), bf16),
            pltpu.VMEM((span + heads, own * keys), bf16),
        ],
        compiler_params=PARAMS,
        name="pack",
    )(me, w_down, cache, queries, gain)


def spread_kernel(x_ref, o_ref):
    half, double = o_ref.shape[1:]
    width = double // 2
    x = x_ref[...].reshape(2 * half, width)
    for j in range(o_ref.shape[0]):
        o_ref[j, :, :width] = x[:half]
        o_ref[j, :, width:] = x[half:]


def spread_rows(arrived, peers):
    experts, cap, width = arrived.shape
    return pl.pallas_call(
        spread_kernel,
        out_shape=shape((peers, experts * cap // 2, 2 * width), bf16),
        in_specs=[VMEM],
        out_specs=VMEM,
        compiler_params=PARAMS,
        name="rows",
    )(arrived)


def down_kernel(me_ref, u_ref, *refs):
    blocks, o_ref, w_ref = refs[:-2], refs[-2], refs[-1]
    peers, _, hid = u_ref.shape
    experts, cap, width = o_ref.shape
    rows, half = experts * cap, hid // 2
    acc = jnp.zeros((rows, width), f32)
    for k in range(peers):
        group = lax.rem(me_ref[0] + (peers - k), peers)
        for t in range(2 * width // 128):
            w_ref[:, 128 * t : 128 * (t + 1)] = blocks[k][half * t : half * (t + 1), :]
        units = u_ref[group, :rows, :]
        acc = acc + jnp.dot(units[:, :half], w_ref[:, :width], preferred_element_type=f32)
        acc = acc + jnp.dot(units[:, half:], w_ref[:, width:], preferred_element_type=f32)
    o_ref[...] = acc.reshape(o_ref.shape).astype(bf16)


def expert_down(me, units, blocks, experts, width):
    hid = units.shape[2]
    return pl.pallas_call(
        down_kernel,
        out_shape=shape((experts, CAP, width), bf16),
        in_specs=[SMEM] + [VMEM] * (1 + len(blocks)),
        out_specs=VMEM,
        scratch_shapes=[pltpu.VMEM((hid // 2, 2 * width), bf16)],
        compiler_params=PARAMS,
        name="down",
    )(me, units, *blocks)


def attend_kernel(me_ref, len_ref, *refs):
    peers = len(refs) - 4
    blocks, (o_ref, m_ref, c_ref, q_ref) = refs[:peers], refs[peers:]
    own, positions, keys = c_ref.shape
    span, heads = positions // peers, q_ref.shape[1] // peers
    me = me_ref[0]
    first = blocks[0].shape[0] - 16 - own * keys // 128 * (span + heads)
    for k in range(peers):
        for t in range(own * keys // 128):
            at = first + t * (span + heads)
            m_ref[:, 128 * t : 128 * (t + 1)] = blocks[k][at : at + span + heads, :]
        for i in range(own):
            c_ref[i, k * span : (k + 1) * span, :] = m_ref[:span, i * keys : (i + 1) * keys]
            q_ref[i, k * heads : (k + 1) * heads, :] = m_ref[span:, i * keys : (i + 1) * keys]
    lane = lax.broadcasted_iota(jnp.int32, (peers * heads, positions), 1)
    block = lax.rem(me + (peers - lane // span), peers)
    position = block * span + lane % span
    for i in range(own):
        live = position < len_ref[me * own + i]
        known = c_ref[i]
        scores = (
            lax.dot_general(
                q_ref[i], known, (((1,), (1,)), ((), ())), preferred_element_type=f32
            )
            * score_scale
        )
        scores = jnp.where(live, scores, -1e30)
        peak = jnp.max(scores, -1, keepdims=True)
        prob = jnp.where(live, jnp.exp(scores - peak), 0.0)
        mass = jnp.sum(prob, -1, keepdims=True)
        out = jnp.dot(prob.astype(bf16), known[:, :LAT], preferred_element_type=f32)
        out = (out / mass).astype(bf16)
        total = peak + jnp.log(mass)
        high = total.astype(bf16).astype(f32)
        middle = (total - high).astype(bf16).astype(f32)
        low = total - high - middle
        tail_lane = lax.broadcasted_iota(jnp.int32, (peers * heads, 128), 1)
        tail = jnp.where(
            tail_lane == 0,
            high,
            jnp.where(tail_lane == 1, middle, jnp.where(tail_lane == 2, low, 0.0)),
        ).astype(bf16)
        for k in range(peers):
            for t in range(LAT // 128 + 1):
                at = (t * own + i) * heads
                piece = tail if t == LAT // 128 else out[:, 128 * t : 128 * (t + 1)]
                o_ref[k, at : at + heads, :] = piece[k * heads : (k + 1) * heads]


def attend(me, lengths, blocks, own, span, heads, keys):
    peers = len(blocks)
    return pl.pallas_call(
        attend_kernel,
        out_shape=shape((peers, own * heads * (LAT // 128 + 1), 128), bf16),
        in_specs=[SMEM, SMEM] + [VMEM] * peers,
        out_specs=VMEM,
        scratch_shapes=[
            pltpu.VMEM((span + heads, own * keys), bf16),
            pltpu.VMEM((own, peers * span, keys), bf16),
            pltpu.VMEM((own, peers * heads, keys), bf16),
        ],
        compiler_params=PARAMS,
        name="attend",
    )(me, lengths, *blocks)


def close_kernel(ret_ref, comb_ref, hid_ref, gain_ref, wdkv_ref, next_ref, small_ref):
    rows = comb_ref.shape[0]
    keys = wdkv_ref.shape[1]
    returned = ret_ref[...].reshape(rows, ret_ref.shape[-1])
    comb = comb_ref[...]
    high = comb.astype(bf16)
    low = (comb - high.astype(f32)).astype(bf16)
    first_dim = (((0,), (0,)), ((), ()))
    moe = lax.dot_general(
        high, returned, first_dim, preferred_element_type=f32
    ) + lax.dot_general(low, returned, first_dim, preferred_element_type=f32)
    result = (hid_ref[...].astype(f32) + moe).astype(bf16)
    next_ref[...] = result
    wide = result.astype(f32)
    square = jnp.sum(wide * wide, -1, keepdims=True)
    first = square.astype(bf16).astype(f32)
    second = (square - first).astype(bf16).astype(f32)
    third = square - first - second
    lane = lax.broadcasted_iota(jnp.int32, (wide.shape[0], small_ref.shape[2] - keys), 1)
    tail = jnp.where(
        lane == 0, first, jnp.where(lane == 1, second, jnp.where(lane == 2, third, 0.0))
    ).astype(bf16)
    down = jnp.dot(
        (wide * gain_ref[...]).astype(bf16), wdkv_ref[...], preferred_element_type=f32
    ).astype(bf16)
    for j in range(small_ref.shape[0]):
        small_ref[j, :, :keys] = down
        small_ref[j, :, keys:] = tail


def close(returned, combine, hidden, gain, w_dkv, peers):
    tokens, width = hidden.shape
    return pl.pallas_call(
        close_kernel,
        out_shape=(
            shape((tokens, width), bf16),
            shape((peers, tokens, w_dkv.shape[1] + 64), bf16),
        ),
        in_specs=[VMEM] * 5,
        out_specs=(VMEM, VMEM),
        compiler_params=PARAMS,
        name="close",
    )(returned, combine, hidden, gain, w_dkv)


def merge_kernel(all_ref, gain_ref, cos_ref, sin_ref, q_ref, units_ref, o_ref, back_ref):
    peers = all_ref.shape[0]
    seqs, heads, lanes = back_ref.shape
    own = seqs // peers
    first = units_ref.shape[1] - own * heads * (lanes // 128)
    for j in range(peers):
        for i in range(own):
            for t in range(lanes // 128):
                at = first + (t * own + i) * heads
                back_ref[j * own + i, :, 128 * t : 128 * (t + 1)] = units_ref[
                    j, at : at + heads, :
                ]
    keys = q_ref.shape[-1]
    total = all_ref[0].astype(f32)
    for j in range(1, all_ref.shape[0]):
        total = total + all_ref[j].astype(f32)
    square = jnp.sum(total[:, keys:], -1, keepdims=True)
    down = total[:, :keys] * lax.rsqrt(square / D + epsilon)
    latent = down[:, :LAT]
    latent = (
        latent
        * lax.rsqrt(jnp.mean(latent * latent, -1, keepdims=True) + epsilon)
        * gain_ref[...]
    )
    rope = down[:, LAT:]
    half = rope.shape[-1] // 2
    turned = jnp.concatenate([rope[:, half:], rope[:, :half]], 1)
    rope = rope * cos_ref[...] + turned * sin_ref[...]
    latent = latent.astype(bf16).astype(f32)[:, None, :]
    rope = rope.astype(bf16).astype(f32)[:, None, :]
    own = (
        jnp.sum(q_ref[:, :, :LAT].astype(f32) * latent, -1, keepdims=True)
        + jnp.sum(q_ref[:, :, LAT:].astype(f32) * rope, -1, keepdims=True)
    ) * score_scale
    cached = jnp.sum(back_ref[:, :, LAT:].astype(f32), -1, keepdims=True)
    peak = jnp.maximum(own, cached)
    own_prob = jnp.exp(own - peak)
    cached_prob = jnp.exp(cached - peak)
    total_prob = own_prob + cached_prob
    o_ref[...] = (
        back_ref[:, :, :LAT].astype(f32) * (cached_prob / total_prob)
        + latent * (own_prob / total_prob)
    ).astype(bf16)


def merge(everything, gain, cos, sin, queries, units):
    seqs, heads, _ = queries.shape
    return pl.pallas_call(
        merge_kernel,
        out_shape=shape((seqs, heads, LAT), bf16),
        in_specs=[VMEM] * 6,
        out_specs=VMEM,
        scratch_shapes=[pltpu.VMEM((seqs, heads, LAT + 128), bf16)],
        compiler_params=PARAMS,
        name="merge",
    )(everything, gain, cos, sin, queries, units)


def mark_kernel(x_ref, o_ref):
    o_ref[...] = x_ref[...]


def mark(x):
    return pl.pallas_call(
        mark_kernel, out_shape=shape(x.shape, x.dtype), in_specs=[VMEM], out_specs=VMEM
    )(x)


def rope_tables(lengths, half):
    inv_freq = 10000.0 ** (-jnp.arange(half, dtype=f32) / half)
    angles = lengths.astype(f32)[:, None] * inv_freq[None, :]
    cos, sin = jnp.cos(angles), jnp.sin(angles)
    return jnp.concatenate([cos, cos], 1), jnp.concatenate([-sin, sin], 1)


def local(
    hidden,
    moe_gain,
    expert_ids,
    slots,
    affinity,
    w_gate,
    w_up,
    w_down,
    attn_gain,
    w_dkv,
    kv_gain,
    queries,
    cache,
    lengths,
):
    seqs, width = hidden.shape
    peers = lax.axis_size("tp")
    experts = lax.axis_size("ep") * lax.axis_size("mb")
    me = lax.axis_index("tp").astype(jnp.int32).reshape(1)

    def moved(x, k):
        return lax.ppermute(x, "tp", [(i, (i + k) % peers) for i in range(peers)])

    send_rows, combine = route(expert_ids, slots, affinity, hidden, experts)
    arrived = exchange(send_rows, ("ep", "mb"))
    blocks = list(pack(me, w_down[0], cache, queries, moe_gain[None], peers))
    for k in MOVES:
        blocks[k] = moved(blocks[k], k)
    attn_gain = mark(attn_gain[None])
    rows = spread_rows(arrived, peers)
    portion = exchange(rows, "tp")
    span, heads, keys = cache.shape[1], queries.shape[1], queries.shape[2]
    attended = attend(me, lengths, blocks, seqs // peers, span, heads, keys)
    units = expert_units(me, portion, w_gate[0], w_up[0], attended, blocks)
    all_units = exchange(units, "tp")
    output = expert_down(me, all_units, blocks, experts, width)
    returned = exchange(output, ("ep", "mb"))
    next_hidden, small = close(returned, combine, hidden, attn_gain, w_dkv, peers)
    everything = exchange(small, "tp")
    cos, sin = rope_tables(lengths, (keys - LAT) // 2)
    latent_out = merge(everything, kv_gain[None], cos, sin, queries, all_units)
    return (next_hidden, latent_out)


def solution(mesh):
    return jax.shard_map(
        local,
        mesh=mesh,
        in_specs=(
            P(("grp", "ep", "mb"), "tp"),
            P("tp"),
            P(("grp", "ep", "mb"), None),
            P(("grp", "ep", "mb"), None),
            P(("grp", "ep", "mb"), None),
            P(("ep", "mb"), None, "tp"),
            P(("ep", "mb"), None, "tp"),
            P(("ep", "mb"), "tp", None),
            P("tp"),
            P("tp", None),
            P(),
            P(("grp", "ep", "mb"), "tp", None),
            P(("grp", "ep", "mb"), "tp", None),
            P(("grp", "ep", "mb")),
        ),
        out_specs=(P(("grp", "ep", "mb"), "tp"), P(("grp", "ep", "mb"), "tp", None)),
        check_vma=False,
    )
```

```python
import jax
import jax.numpy as jnp
from jax import lax
from jax.experimental import pallas as pl
from jax.experimental.pallas import tpu as pltpu
from jax.sharding import PartitionSpec as P


D = 3584
LAT = 512
CAP = 8
MOVES = (4, 3, 5, 2, 6, 1, 7)

epsilon = 1e-06
route_scale = 2.5
score_scale = 192.0 ** (-0.5)
f32 = jnp.float32
bf16 = jnp.bfloat16
VMEM = pl.BlockSpec(memory_space=pltpu.VMEM)
SMEM = pl.BlockSpec(memory_space=pltpu.SMEM)
HBM = pl.BlockSpec(memory_space=pltpu.HBM)
PARAMS = pltpu.CompilerParams(vmem_limit_bytes=40 * 1024 * 1024)


def shape(dims, dtype):
    return jax.ShapeDtypeStruct(dims, dtype)


def exchange(x, axis):
    return lax.all_to_all(x, axis, split_axis=0, concat_axis=0, tiled=True)


def ahead(me_ref, k, peers):
    return lax.rem(me_ref[0] + me_ref[1] * k + peers, peers)


def behind(me_ref, k, peers):
    return lax.rem(me_ref[0] - me_ref[1] * k + peers, peers)


def in_hbm(x):
    return pltpu.with_memory_space_constraint(x, pltpu.HBM)


def fetch(sources, targets, sems):
    copies = [
        pltpu.make_async_copy(source, target, sems.at[i])
        for i, (source, target) in enumerate(zip(sources, targets))
    ]
    for copy in copies:
        copy.start()
    return copies


def route_kernel(ids_hbm, slots_hbm, aff_hbm, hid_hbm, send_ref, comb_ref, *refs):
    ids_ref, slots_ref, aff_ref, hid_ref, sems = refs
    copies = fetch((ids_hbm, slots_hbm, aff_hbm, hid_hbm), refs[:4], sems)
    for copy in copies:
        copy.wait()
    experts = send_ref.shape[0]
    top, tokens = ids_ref.shape
    rows = experts * CAP
    slots = slots_ref[...]
    affinity = aff_ref[...]
    weight = route_scale * affinity / jnp.sum(affinity, 0, keepdims=True)
    target = jnp.where(slots < CAP, ids_ref[...] * CAP + slots, -1)
    row = lax.broadcasted_iota(jnp.int32, (rows, tokens), 0)
    pick = jnp.zeros((rows, tokens), f32)
    comb = jnp.zeros((rows, tokens), f32)
    for k in range(top):
        match = target[k : k + 1, :] == row
        pick = jnp.where(match, 1.0, pick)
        comb = jnp.where(match, weight[k : k + 1, :], comb)
    comb_ref[...] = comb
    sent = jnp.dot(pick.astype(bf16), hid_ref[...], preferred_element_type=f32)
    send_ref[...] = sent.reshape(send_ref.shape).astype(bf16)


def route(expert_ids, slots, affinity, hidden, experts):
    tokens, width = hidden.shape
    inputs = (expert_ids.T, slots.T, affinity.T, hidden)
    return pl.pallas_call(
        route_kernel,
        out_shape=(shape((experts, CAP, width), bf16), shape((experts * CAP, tokens), f32)),
        in_specs=[HBM] * 4,
        out_specs=(VMEM, VMEM),
        scratch_shapes=[pltpu.VMEM(x.shape, x.dtype) for x in inputs]
        + [pltpu.SemaphoreType.DMA((4,))],
        compiler_params=PARAMS,
        name="route",
    )(*[in_hbm(x) for x in inputs])


def gain_of(block, at, width):
    rows = block[at : at + 16, :].astype(f32)
    tiles = (width + 127) // 128
    total = rows[:tiles] + rows[tiles : 2 * tiles] + rows[2 * tiles : 3 * tiles]
    return [total[q : q + 1, : min(128, width - 128 * q)] for q in range(tiles)]


def units_kernel(me_ref, wg_hbm, wu_hbm, att_ref, *refs):
    peers = att_ref.shape[0]
    blocks, parts = refs[:peers], refs[peers : 2 * peers + 1]
    o_ref, wg_ref, wu_ref, n_ref, g_ref, u_ref, sems = refs[2 * peers + 1 :]
    copies = fetch((wg_hbm, wu_hbm), (wg_ref, wu_ref), sems)
    half, double = parts[0].shape
    rows, cols, middle = 2 * half, double // 2, peers // 2
    square = jnp.zeros((rows, 1), f32)
    for k in range(peers):
        at = 0
        for part in parts[k : k + 1] if k < middle else parts[k : k + 2] if k == middle else parts[k + 1 : k + 2]:
            end = at + part.shape[0]
            n_ref[k, at:end, :] = part[:, :cols]
            n_ref[k, half + at : half + end, :] = part[:, cols:]
            at = end
        x = n_ref[k].astype(f32)
        square = square + jnp.sum(x * x, -1, keepdims=True)
    scale = lax.rsqrt(square / D + epsilon)
    copies[0].wait()
    copies[1].wait()
    for k in range(peers):
        j = behind(me_ref, k, peers)
        gain = jnp.concatenate(gain_of(blocks[k], blocks[k].shape[0] - 16, cols), 1)
        normed = (n_ref[k].astype(f32) * scale * gain).astype(bf16)
        part = pl.ds(pl.multiple_of(j * cols, 64), cols)
        gate = jnp.dot(normed, wg_ref[part, :], preferred_element_type=f32)
        up = jnp.dot(normed, wu_ref[part, :], preferred_element_type=f32)
        if k == 0:
            g_ref[...] = gate
            u_ref[...] = up
        else:
            g_ref[...] += gate
            u_ref[...] += up
        o_ref[j, rows:, :] = att_ref[k]
    gate = g_ref[...]
    units = (gate / (1.0 + jnp.exp(-gate)) * u_ref[...]).astype(bf16)
    for j in range(peers):
        o_ref[j, :rows, :] = units


def expert_units(me, parts, w_gate, w_up, attended, blocks):
    peers = len(blocks)
    half, double = parts[0].shape
    rows, cols, hid = 2 * half, double // 2, w_gate.shape[1]
    return pl.pallas_call(
        units_kernel,
        out_shape=shape((peers, rows + attended.shape[1], hid), bf16),
        in_specs=[SMEM, HBM, HBM] + [VMEM] * (2 * peers + 2),
        out_specs=VMEM,
        scratch_shapes=[
            pltpu.VMEM(w_gate.shape, bf16),
            pltpu.VMEM(w_up.shape, bf16),
            pltpu.VMEM((peers, rows, cols), bf16),
            pltpu.VMEM((rows, hid), f32),
            pltpu.VMEM((rows, hid), f32),
            pltpu.SemaphoreType.DMA((2,)),
        ],
        compiler_params=PARAMS,
        name="units",
    )(me, in_hbm(w_gate), in_hbm(w_up), attended, *blocks, *parts)


def pack_kernel(me_ref, wd_hbm, cache_hbm, q_hbm, gain_ref, *refs):
    outs, (wd_ref, cache_ref, q_ref, tiles_ref, keys_ref, sems) = refs[:-6], refs[-6:]
    copies = fetch((wd_hbm, cache_hbm, q_hbm), (wd_ref, cache_ref, q_ref), sems)
    peers = len(outs)
    half, double = tiles_ref.shape[1:]
    width = double // 2
    span, heads, keys = cache_ref.shape[1], q_ref.shape[1], cache_ref.shape[2]
    own = cache_ref.shape[0] // peers
    copies[0].wait()
    for j in range(peers):
        tiles_ref[j, :, :width] = wd_ref[:half, j * width : (j + 1) * width]
        tiles_ref[j, :, width:] = wd_ref[half:, j * width : (j + 1) * width]
    gain = gain_ref[...]
    first = gain.astype(bf16).astype(f32)
    second = (gain - first).astype(bf16).astype(f32)
    row = lax.broadcasted_iota(jnp.int32, (16, 128), 0)
    packed = jnp.zeros((16, 128), f32)
    tiles = (width + 127) // 128
    for p, value in enumerate((first, second, gain - first - second)):
        for q in range(tiles):
            piece = value[:, 128 * q : min(128 * (q + 1), width)]
            if piece.shape[1] < 128:
                piece = jnp.concatenate([piece, jnp.zeros((1, 128 - piece.shape[1]), f32)], 1)
            packed = jnp.where(row == p * tiles + q, piece, packed)
    packed = packed.astype(bf16)
    copies[1].wait()
    copies[2].wait()
    for k in range(peers):
        to = ahead(me_ref, k, peers)
        at = 0
        for t in range(double // 128):
            outs[k][at : at + half, :] = tiles_ref[to, :, 128 * t : 128 * (t + 1)]
            at += half
        for i in range(own):
            keys_ref[:span, i * keys : (i + 1) * keys] = cache_ref[to * own + i]
            keys_ref[span:, i * keys : (i + 1) * keys] = q_ref[to * own + i]
        for t in range(own * keys // 128):
            outs[k][at : at + span + heads, :] = keys_ref[:, 128 * t : 128 * (t + 1)]
            at += span + heads
        outs[k][at : at + 16, :] = packed


def pack(me, w_down, cache, queries, gain, peers):
    hid, width = w_down.shape[0], w_down.shape[1] // peers
    seqs, span, keys = cache.shape
    own, heads = seqs // peers, queries.shape[1]
    rows = hid * width // 128 + own * (span + heads) * keys // 128 + 16
    return pl.pallas_call(
        pack_kernel,
        out_shape=tuple(shape((rows, 128), bf16) for _ in range(peers)),
        in_specs=[SMEM] + [HBM] * 3 + [VMEM],
        out_specs=tuple(VMEM for _ in range(peers)),
        scratch_shapes=[
            pltpu.VMEM(w_down.shape, bf16),
            pltpu.VMEM(cache.shape, bf16),
            pltpu.VMEM(queries.shape, bf16),
            pltpu.VMEM((peers, hid // 2, 2 * width), bf16),
            pltpu.VMEM((span + heads, own * keys), bf16),
            pltpu.SemaphoreType.DMA((3,)),
        ],
        compiler_params=PARAMS,
        name="pack",
    )(me, in_hbm(w_down), in_hbm(cache), in_hbm(queries), gain)


def rows_kernel(x_ref, o_ref):
    half, double = o_ref.shape
    width = double // 2
    x = x_ref[...].reshape(2 * half, width)
    o_ref[:, :width] = x[:half]
    o_ref[:, width:] = x[half:]


def packed_rows(arrived):
    experts, cap, width = arrived.shape
    return pl.pallas_call(
        rows_kernel,
        out_shape=shape((experts * cap // 2, 2 * width), bf16),
        in_specs=[VMEM],
        out_specs=VMEM,
        compiler_params=PARAMS,
        name="rows",
    )(arrived)


def ring(x, moved, peers):
    steps, half = peers // 2, x.shape[0] // 2
    there, back = [x], [x]
    for _ in range(1, steps):
        there.append(moved(there[-1], 1))
        back.append(moved(back[-1], peers - 1))
    upper = moved(there[-1][:half], 1)
    lower = moved(back[-1][half:], peers - 1)
    return there + [upper, lower] + back[:0:-1]


def down_kernel(me_ref, u_ref, *refs):
    blocks, o_ref, w_ref = refs[:-2], refs[-2], refs[-1]
    peers, _, hid = u_ref.shape
    experts, cap, width = o_ref.shape
    rows, half = experts * cap, hid // 2
    acc = jnp.zeros((rows, width), f32)
    for k in range(peers):
        group = behind(me_ref, k, peers)
        for t in range(2 * width // 128):
            w_ref[:, 128 * t : 128 * (t + 1)] = blocks[k][half * t : half * (t + 1), :]
        units = u_ref[group, :rows, :]
        acc = acc + jnp.dot(units[:, :half], w_ref[:, :width], preferred_element_type=f32)
        acc = acc + jnp.dot(units[:, half:], w_ref[:, width:], preferred_element_type=f32)
    o_ref[...] = acc.reshape(o_ref.shape).astype(bf16)


def expert_down(me, units, blocks, experts, width):
    hid = units.shape[2]
    return pl.pallas_call(
        down_kernel,
        out_shape=shape((experts, CAP, width), bf16),
        in_specs=[SMEM] + [VMEM] * (1 + len(blocks)),
        out_specs=VMEM,
        scratch_shapes=[pltpu.VMEM((hid // 2, 2 * width), bf16)],
        compiler_params=PARAMS,
        name="down",
    )(me, units, *blocks)


def attend_kernel(me_ref, len_ref, *refs):
    peers = len(refs) - 4
    blocks, (o_ref, m_ref, c_ref, q_ref) = refs[:peers], refs[peers:]
    own, positions, keys = c_ref.shape
    span, heads = positions // peers, q_ref.shape[1] // peers
    me = me_ref[0]
    first = blocks[0].shape[0] - 16 - own * keys // 128 * (span + heads)
    for k in range(peers):
        for t in range(own * keys // 128):
            at = first + t * (span + heads)
            m_ref[:, 128 * t : 128 * (t + 1)] = blocks[k][at : at + span + heads, :]
        for i in range(own):
            c_ref[i, k * span : (k + 1) * span, :] = m_ref[:span, i * keys : (i + 1) * keys]
            q_ref[i, k * heads : (k + 1) * heads, :] = m_ref[span:, i * keys : (i + 1) * keys]
    lane = lax.broadcasted_iota(jnp.int32, (peers * heads, positions), 1)
    block = behind(me_ref, lane // span, peers)
    position = block * span + lane % span
    for i in range(own):
        live = position < len_ref[me * own + i]
        known = c_ref[i]
        scores = (
            lax.dot_general(
                q_ref[i], known, (((1,), (1,)), ((), ())), preferred_element_type=f32
            )
            * score_scale
        )
        scores = jnp.where(live, scores, -1e30)
        peak = jnp.max(scores, -1, keepdims=True)
        prob = jnp.where(live, jnp.exp(scores - peak), 0.0)
        mass = jnp.sum(prob, -1, keepdims=True)
        out = jnp.dot(prob.astype(bf16), known[:, :LAT], preferred_element_type=f32)
        out = (out / mass).astype(bf16)
        total = peak + jnp.log(mass)
        high = total.astype(bf16).astype(f32)
        middle = (total - high).astype(bf16).astype(f32)
        low = total - high - middle
        tail_lane = lax.broadcasted_iota(jnp.int32, (peers * heads, 128), 1)
        tail = jnp.where(
            tail_lane == 0,
            high,
            jnp.where(tail_lane == 1, middle, jnp.where(tail_lane == 2, low, 0.0)),
        ).astype(bf16)
        for k in range(peers):
            for t in range(LAT // 128 + 1):
                at = (t * own + i) * heads
                piece = tail if t == LAT // 128 else out[:, 128 * t : 128 * (t + 1)]
                o_ref[k, at : at + heads, :] = piece[k * heads : (k + 1) * heads]


def attend(me, lengths, blocks, own, span, heads, keys):
    peers = len(blocks)
    return pl.pallas_call(
        attend_kernel,
        out_shape=shape((peers, own * heads * (LAT // 128 + 1), 128), bf16),
        in_specs=[SMEM, SMEM] + [VMEM] * peers,
        out_specs=VMEM,
        scratch_shapes=[
            pltpu.VMEM((span + heads, own * keys), bf16),
            pltpu.VMEM((own, peers * span, keys), bf16),
            pltpu.VMEM((own, peers * heads, keys), bf16),
        ],
        compiler_params=PARAMS,
        name="attend",
    )(me, lengths, *blocks)


def close_kernel(ret_ref, comb_ref, hid_ref, gain_ref, wdkv_ref, next_ref, small_ref):
    rows = comb_ref.shape[0]
    keys = wdkv_ref.shape[1]
    returned = ret_ref[...].reshape(rows, ret_ref.shape[-1])
    comb = comb_ref[...]
    high = comb.astype(bf16)
    low = (comb - high.astype(f32)).astype(bf16)
    first_dim = (((0,), (0,)), ((), ()))
    moe = lax.dot_general(
        high, returned, first_dim, preferred_element_type=f32
    ) + lax.dot_general(low, returned, first_dim, preferred_element_type=f32)
    result = (hid_ref[...].astype(f32) + moe).astype(bf16)
    next_ref[...] = result
    wide = result.astype(f32)
    square = jnp.sum(wide * wide, -1, keepdims=True)
    first = square.astype(bf16).astype(f32)
    second = (square - first).astype(bf16).astype(f32)
    third = square - first - second
    lane = lax.broadcasted_iota(jnp.int32, (wide.shape[0], small_ref.shape[2] - keys), 1)
    tail = jnp.where(
        lane == 0, first, jnp.where(lane == 1, second, jnp.where(lane == 2, third, 0.0))
    ).astype(bf16)
    down = jnp.dot(
        (wide * gain_ref[...]).astype(bf16), wdkv_ref[...], preferred_element_type=f32
    ).astype(bf16)
    for j in range(small_ref.shape[0]):
        small_ref[j, :, :keys] = down
        small_ref[j, :, keys:] = tail


def close(returned, combine, hidden, gain, w_dkv, peers):
    tokens, width = hidden.shape
    return pl.pallas_call(
        close_kernel,
        out_shape=(
            shape((tokens, width), bf16),
            shape((peers, tokens, w_dkv.shape[1] + 64), bf16),
        ),
        in_specs=[VMEM] * 5,
        out_specs=(VMEM, VMEM),
        compiler_params=PARAMS,
        name="close",
    )(returned, combine, hidden, gain, w_dkv)


def merge_kernel(all_ref, gain_ref, cos_ref, sin_ref, q_ref, units_ref, o_ref, back_ref):
    peers = all_ref.shape[0]
    seqs, heads, lanes = back_ref.shape
    own = seqs // peers
    first = units_ref.shape[1] - own * heads * (lanes // 128)
    for j in range(peers):
        for i in range(own):
            for t in range(lanes // 128):
                at = first + (t * own + i) * heads
                back_ref[j * own + i, :, 128 * t : 128 * (t + 1)] = units_ref[
                    j, at : at + heads, :
                ]
    keys = q_ref.shape[-1]
    total = all_ref[0].astype(f32)
    for j in range(1, all_ref.shape[0]):
        total = total + all_ref[j].astype(f32)
    square = jnp.sum(total[:, keys:], -1, keepdims=True)
    down = total[:, :keys] * lax.rsqrt(square / D + epsilon)
    latent = down[:, :LAT]
    latent = (
        latent
        * lax.rsqrt(jnp.mean(latent * latent, -1, keepdims=True) + epsilon)
        * gain_ref[...]
    )
    rope = down[:, LAT:]
    half = rope.shape[-1] // 2
    turned = jnp.concatenate([rope[:, half:], rope[:, :half]], 1)
    rope = rope * cos_ref[...] + turned * sin_ref[...]
    latent = latent.astype(bf16).astype(f32)[:, None, :]
    rope = rope.astype(bf16).astype(f32)[:, None, :]
    own = (
        jnp.sum(q_ref[:, :, :LAT].astype(f32) * latent, -1, keepdims=True)
        + jnp.sum(q_ref[:, :, LAT:].astype(f32) * rope, -1, keepdims=True)
    ) * score_scale
    cached = jnp.sum(back_ref[:, :, LAT:].astype(f32), -1, keepdims=True)
    peak = jnp.maximum(own, cached)
    own_prob = jnp.exp(own - peak)
    cached_prob = jnp.exp(cached - peak)
    total_prob = own_prob + cached_prob
    o_ref[...] = (
        back_ref[:, :, :LAT].astype(f32) * (cached_prob / total_prob)
        + latent * (own_prob / total_prob)
    ).astype(bf16)


def merge(everything, gain, cos, sin, queries, units):
    seqs, heads, _ = queries.shape
    return pl.pallas_call(
        merge_kernel,
        out_shape=shape((seqs, heads, LAT), bf16),
        in_specs=[VMEM] * 6,
        out_specs=VMEM,
        scratch_shapes=[pltpu.VMEM((seqs, heads, LAT + 128), bf16)],
        compiler_params=PARAMS,
        name="merge",
    )(everything, gain, cos, sin, queries, units)


def rope_tables(lengths, half):
    inv_freq = 10000.0 ** (-jnp.arange(half, dtype=f32) / half)
    angles = lengths.astype(f32)[:, None] * inv_freq[None, :]
    cos, sin = jnp.cos(angles), jnp.sin(angles)
    return jnp.concatenate([cos, cos], 1), jnp.concatenate([-sin, sin], 1)


def local(
    hidden,
    moe_gain,
    expert_ids,
    slots,
    affinity,
    w_gate,
    w_up,
    w_down,
    attn_gain,
    w_dkv,
    kv_gain,
    queries,
    cache,
    lengths,
):
    seqs, width = hidden.shape
    peers = lax.axis_size("tp")
    experts = lax.axis_size("ep") * lax.axis_size("mb")
    cores = lax.axis_size("mb")
    sense = 1 - 2 * (lax.axis_index("mb") % 2)
    me = jnp.stack([lax.axis_index("tp"), sense]).astype(jnp.int32)

    def moved(x, k):
        pairs = [
            (i * cores + c, (i + (k if c % 2 == 0 else peers - k)) % peers * cores + c)
            for i in range(peers)
            for c in range(cores)
        ]
        return lax.ppermute(x, ("tp", "mb"), pairs)

    send_rows, combine = route(expert_ids, slots, affinity, hidden, experts)
    arrived = exchange(send_rows, ("ep", "mb"))
    blocks = list(pack(me, w_down[0], cache, queries, moe_gain[None], peers))
    for k in MOVES:
        blocks[k] = moved(blocks[k], k)
    parts = ring(packed_rows(arrived), moved, peers)
    span, heads, keys = cache.shape[1], queries.shape[1], queries.shape[2]
    attended = attend(me, lengths, blocks, seqs // peers, span, heads, keys)
    units = expert_units(me, parts, w_gate[0], w_up[0], attended, blocks)
    all_units = exchange(units, "tp")
    output = expert_down(me, all_units, blocks, experts, width)
    returned = exchange(output, ("ep", "mb"))
    next_hidden, small = close(returned, combine, hidden, attn_gain[None], w_dkv, peers)
    everything = exchange(small, "tp")
    cos, sin = rope_tables(lengths, (keys - LAT) // 2)
    latent_out = merge(everything, kv_gain[None], cos, sin, queries, all_units)
    return (next_hidden, latent_out)


def solution(mesh):
    return jax.shard_map(
        local,
        mesh=mesh,
        in_specs=(
            P(("grp", "ep", "mb"), "tp"),
            P("tp"),
            P(("grp", "ep", "mb"), None),
            P(("grp", "ep", "mb"), None),
            P(("grp", "ep", "mb"), None),
            P(("ep", "mb"), None, "tp"),
            P(("ep", "mb"), None, "tp"),
            P(("ep", "mb"), "tp", None),
            P("tp"),
            P("tp", None),
            P(),
            P(("grp", "ep", "mb"), "tp", None),
            P(("grp", "ep", "mb"), "tp", None),
            P(("grp", "ep", "mb")),
        ),
        out_specs=(P(("grp", "ep", "mb"), "tp"), P(("grp", "ep", "mb"), "tp", None)),
        check_vma=False,
    )
```

```python
import jax
import jax.numpy as jnp
from jax import lax
from jax.experimental import pallas as pl
from jax.experimental.pallas import tpu as pltpu
from jax.sharding import PartitionSpec as P


D = 3584
LAT = 512
CAP = 8
EARLY = (4, 3, 5, 2)
LATE = (6, 1, 7)
GAIN_ROWS = 8

epsilon = 1e-06
route_scale = 2.5
score_scale = 192.0 ** (-0.5)
f32 = jnp.float32
bf16 = jnp.bfloat16
VMEM = pl.BlockSpec(memory_space=pltpu.VMEM)
SMEM = pl.BlockSpec(memory_space=pltpu.SMEM)
HBM = pl.BlockSpec(memory_space=pltpu.HBM)
PARAMS = pltpu.CompilerParams(vmem_limit_bytes=40 * 1024 * 1024)


def shape(dims, dtype):
    return jax.ShapeDtypeStruct(dims, dtype)


def exchange(x, axis):
    return lax.all_to_all(x, axis, split_axis=0, concat_axis=0, tiled=True)


def in_hbm(x):
    return pltpu.with_memory_space_constraint(x, pltpu.HBM)


def fetch(sources, targets, sems):
    copies = [
        pltpu.make_async_copy(source, target, sems.at[i])
        for i, (source, target) in enumerate(zip(sources, targets))
    ]
    for copy in copies:
        copy.start()
    return copies


def route_kernel(ids_hbm, slots_hbm, aff_hbm, hid_hbm, send_ref, comb_ref, *refs):
    ids_ref, slots_ref, aff_ref, hid_ref, sems = refs
    copies = fetch((ids_hbm, slots_hbm, aff_hbm, hid_hbm), refs[:4], sems)
    for copy in copies:
        copy.wait()
    experts = send_ref.shape[0]
    top, tokens = ids_ref.shape
    rows = experts * CAP
    slots = slots_ref[...]
    affinity = aff_ref[...]
    weight = route_scale * affinity / jnp.sum(affinity, 0, keepdims=True)
    target = jnp.where(slots < CAP, ids_ref[...] * CAP + slots, -1)
    row = lax.broadcasted_iota(jnp.int32, (rows, tokens), 0)
    pick = jnp.zeros((rows, tokens), f32)
    comb = jnp.zeros((rows, tokens), f32)
    for k in range(top):
        match = target[k : k + 1, :] == row
        pick = jnp.where(match, 1.0, pick)
        comb = jnp.where(match, weight[k : k + 1, :], comb)
    comb_ref[...] = comb
    sent = jnp.dot(pick.astype(bf16), hid_ref[...], preferred_element_type=f32)
    send_ref[...] = sent.reshape(send_ref.shape).astype(bf16)


def route(expert_ids, slots, affinity, hidden, experts):
    tokens, width = hidden.shape
    inputs = (expert_ids.T, slots.T, affinity.T, hidden)
    return pl.pallas_call(
        route_kernel,
        out_shape=(shape((experts, CAP, width), bf16), shape((experts * CAP, tokens), f32)),
        in_specs=[HBM] * 4,
        out_specs=(VMEM, VMEM),
        scratch_shapes=[pltpu.VMEM(x.shape, x.dtype) for x in inputs]
        + [pltpu.SemaphoreType.DMA((4,))],
        compiler_params=PARAMS,
        name="route",
    )(*[in_hbm(x) for x in inputs])


def units_kernel(me_ref, wg_hbm, wu_hbm, *refs):
    parts = refs[:-7]
    o_ref, wg_ref, wu_ref, n_ref, g_ref, u_ref, sems = refs[-7:]
    copies = fetch((wg_hbm, wu_hbm), (wg_ref, wu_ref), sems)
    peers, rows, cols = n_ref.shape
    half, middle = rows // 2, peers // 2
    square = jnp.zeros((rows, 1), f32)
    gains = []
    for k in range(peers):
        first = k if k <= middle else k + 1
        at = 0
        for part in parts[first : first + (2 if k == middle else 1)]:
            end = min(at + part.shape[0], half)
            n_ref[k, at:end, :] = part[: end - at, :cols]
            n_ref[k, half + at : half + end, :] = part[: end - at, cols:]
            if at + part.shape[0] > half:
                gains.append(jnp.sum(part[end - at :, :cols].astype(f32), 0, keepdims=True))
            at = end
        x = n_ref[k].astype(f32)
        square = square + jnp.sum(x * x, -1, keepdims=True)
    scale = lax.rsqrt(square / D + epsilon)
    copies[0].wait()
    copies[1].wait()
    for k in range(peers):
        j = lax.rem(me_ref[0] + (peers - k), peers)
        normed = (n_ref[k].astype(f32) * scale * gains[k]).astype(bf16)
        part = pl.ds(pl.multiple_of(j * cols, 64), cols)
        gate = jnp.dot(normed, wg_ref[part, :], preferred_element_type=f32)
        up = jnp.dot(normed, wu_ref[part, :], preferred_element_type=f32)
        if k == 0:
            g_ref[...] = gate
            u_ref[...] = up
        else:
            g_ref[...] += gate
            u_ref[...] += up
    gate = g_ref[...]
    units = (gate / (1.0 + jnp.exp(-gate)) * u_ref[...]).astype(bf16)
    for j in range(peers):
        o_ref[j] = units


def expert_units(me, parts, w_gate, w_up, peers):
    half, cols, hid = parts[0].shape[0] - GAIN_ROWS, parts[0].shape[1] // 2, w_gate.shape[1]
    rows = 2 * half
    return pl.pallas_call(
        units_kernel,
        out_shape=shape((peers, rows, hid), bf16),
        in_specs=[SMEM, HBM, HBM] + [VMEM] * len(parts),
        out_specs=VMEM,
        scratch_shapes=[
            pltpu.VMEM(w_gate.shape, bf16),
            pltpu.VMEM(w_up.shape, bf16),
            pltpu.VMEM((peers, rows, cols), bf16),
            pltpu.VMEM((rows, hid), f32),
            pltpu.VMEM((rows, hid), f32),
            pltpu.SemaphoreType.DMA((2,)),
        ],
        compiler_params=PARAMS,
        name="units",
    )(me, in_hbm(w_gate), in_hbm(w_up), *parts)


def pack_kernel(me_ref, wd_hbm, cache_hbm, q_hbm, *refs):
    outs, (wd_ref, cache_ref, q_ref, tiles_ref, keys_ref, sems) = refs[:-6], refs[-6:]
    copies = fetch((wd_hbm, cache_hbm, q_hbm), (wd_ref, cache_ref, q_ref), sems)
    peers = len(outs)
    half, double = tiles_ref.shape[1:]
    width = double // 2
    span, heads, keys = cache_ref.shape[1], q_ref.shape[1], cache_ref.shape[2]
    own = cache_ref.shape[0] // peers
    copies[0].wait()
    for j in range(peers):
        tiles_ref[j, :, :width] = wd_ref[:half, j * width : (j + 1) * width]
        tiles_ref[j, :, width:] = wd_ref[half:, j * width : (j + 1) * width]
    copies[1].wait()
    copies[2].wait()
    for k in range(peers):
        to = lax.rem(me_ref[0] + k, peers)
        at = 0
        for t in range(double // 128):
            outs[k][at : at + half, :] = tiles_ref[to, :, 128 * t : 128 * (t + 1)]
            at += half
        for i in range(own):
            keys_ref[:span, i * keys : (i + 1) * keys] = cache_ref[to * own + i]
            keys_ref[span:, i * keys : (i + 1) * keys] = q_ref[to * own + i]
        for t in range(own * keys // 128):
            outs[k][at : at + span + heads, :] = keys_ref[:, 128 * t : 128 * (t + 1)]
            at += span + heads


def pack(me, w_down, cache, queries, peers):
    hid, width = w_down.shape[0], w_down.shape[1] // peers
    seqs, span, keys = cache.shape
    own, heads = seqs // peers, queries.shape[1]
    rows = hid * width // 128 + own * (span + heads) * keys // 128
    return pl.pallas_call(
        pack_kernel,
        out_shape=tuple(shape((rows, 128), bf16) for _ in range(peers)),
        in_specs=[SMEM] + [HBM] * 3,
        out_specs=tuple(VMEM for _ in range(peers)),
        scratch_shapes=[
            pltpu.VMEM(w_down.shape, bf16),
            pltpu.VMEM(cache.shape, bf16),
            pltpu.VMEM(queries.shape, bf16),
            pltpu.VMEM((peers, hid // 2, 2 * width), bf16),
            pltpu.VMEM((span + heads, own * keys), bf16),
            pltpu.SemaphoreType.DMA((3,)),
        ],
        compiler_params=PARAMS,
        name="pack",
    )(me, in_hbm(w_down), in_hbm(cache), in_hbm(queries))


def rows_kernel(x_ref, gain_ref, o_ref):
    half, width = o_ref.shape[0] - GAIN_ROWS, o_ref.shape[1] // 2
    x = x_ref[...].reshape(2 * half, width)
    o_ref[:half, :width] = x[:half]
    o_ref[:half, width:] = x[half:]
    gain = gain_ref[...]
    first = gain.astype(bf16).astype(f32)
    second = (gain - first).astype(bf16).astype(f32)
    third = gain - first - second
    row = lax.broadcasted_iota(jnp.int32, (GAIN_ROWS, width), 0)
    parts = jnp.where(
        row == 0, first, jnp.where(row == 1, second, jnp.where(row == 2, third, 0.0))
    ).astype(bf16)
    o_ref[half:, :width] = parts
    o_ref[half:, width:] = parts


def packed_rows(arrived, gain):
    experts, cap, width = arrived.shape
    return pl.pallas_call(
        rows_kernel,
        out_shape=shape((experts * cap // 2 + GAIN_ROWS, 2 * width), bf16),
        in_specs=[VMEM] * 2,
        out_specs=VMEM,
        compiler_params=PARAMS,
        name="rows",
    )(arrived, gain)


def ring(x, moved, peers):
    steps, cut = peers // 2, (x.shape[0] // 2 + 7) // 8 * 8
    there, back = [x], [x]
    for _ in range(1, steps):
        there.append(moved(there[-1], 1))
        back.append(moved(back[-1], peers - 1))
    upper = moved(there[-1][:cut], 1)
    lower = moved(back[-1][cut:], peers - 1)
    return there + [upper, lower] + back[:0:-1]


def down_kernel(me_ref, u_ref, *refs):
    blocks, o_ref, w_ref = refs[:-2], refs[-2], refs[-1]
    peers, _, hid = u_ref.shape
    experts, cap, width = o_ref.shape
    rows, half = experts * cap, hid // 2
    acc = jnp.zeros((rows, width), f32)
    for k in range(peers):
        group = lax.rem(me_ref[0] + (peers - k), peers)
        for t in range(2 * width // 128):
            w_ref[:, 128 * t : 128 * (t + 1)] = blocks[k][half * t : half * (t + 1), :]
        units = u_ref[group, :rows, :]
        acc = acc + jnp.dot(units[:, :half], w_ref[:, :width], preferred_element_type=f32)
        acc = acc + jnp.dot(units[:, half:], w_ref[:, width:], preferred_element_type=f32)
    o_ref[...] = acc.reshape(o_ref.shape).astype(bf16)


def expert_down(me, units, blocks, experts, width):
    hid = units.shape[2]
    return pl.pallas_call(
        down_kernel,
        out_shape=shape((experts, CAP, width), bf16),
        in_specs=[SMEM] + [VMEM] * (1 + len(blocks)),
        out_specs=VMEM,
        scratch_shapes=[pltpu.VMEM((hid // 2, 2 * width), bf16)],
        compiler_params=PARAMS,
        name="down",
    )(me, units, *blocks)


def attend_kernel(me_ref, len_ref, *refs):
    peers = len(refs) - 4
    blocks, (o_ref, m_ref, c_ref, q_ref) = refs[:peers], refs[peers:]
    own, positions, keys = c_ref.shape
    span, heads = positions // peers, q_ref.shape[1] // peers
    me = me_ref[0]
    first = blocks[0].shape[0] - own * keys // 128 * (span + heads)
    for k in range(peers):
        for t in range(own * keys // 128):
            at = first + t * (span + heads)
            m_ref[:, 128 * t : 128 * (t + 1)] = blocks[k][at : at + span + heads, :]
        for i in range(own):
            c_ref[i, k * span : (k + 1) * span, :] = m_ref[:span, i * keys : (i + 1) * keys]
            q_ref[i, k * heads : (k + 1) * heads, :] = m_ref[span:, i * keys : (i + 1) * keys]
    lane = lax.broadcasted_iota(jnp.int32, (peers * heads, positions), 1)
    block = lax.rem(me + (peers - lane // span), peers)
    position = block * span + lane % span
    for i in range(own):
        live = position < len_ref[me * own + i]
        known = c_ref[i]
        scores = (
            lax.dot_general(
                q_ref[i], known, (((1,), (1,)), ((), ())), preferred_element_type=f32
            )
            * score_scale
        )
        scores = jnp.where(live, scores, -1e30)
        peak = jnp.max(scores, -1, keepdims=True)
        prob = jnp.where(live, jnp.exp(scores - peak), 0.0)
        mass = jnp.sum(prob, -1, keepdims=True)
        out = jnp.dot(prob.astype(bf16), known[:, :LAT], preferred_element_type=f32)
        out = (out / mass).astype(bf16)
        total = peak + jnp.log(mass)
        high = total.astype(bf16).astype(f32)
        middle = (total - high).astype(bf16).astype(f32)
        low = total - high - middle
        tail_lane = lax.broadcasted_iota(jnp.int32, (peers * heads, 128), 1)
        tail = jnp.where(
            tail_lane == 0,
            high,
            jnp.where(tail_lane == 1, middle, jnp.where(tail_lane == 2, low, 0.0)),
        ).astype(bf16)
        for k in range(peers):
            o_ref[k, i * heads : (i + 1) * heads, :LAT] = out[k * heads : (k + 1) * heads]
            o_ref[k, i * heads : (i + 1) * heads, LAT:] = tail[k * heads : (k + 1) * heads]


def attend(me, lengths, blocks, own, span, heads, keys):
    peers = len(blocks)
    return pl.pallas_call(
        attend_kernel,
        out_shape=shape((peers, own * heads, LAT + 128), bf16),
        in_specs=[SMEM, SMEM] + [VMEM] * peers,
        out_specs=VMEM,
        scratch_shapes=[
            pltpu.VMEM((span + heads, own * keys), bf16),
            pltpu.VMEM((own, peers * span, keys), bf16),
            pltpu.VMEM((own, peers * heads, keys), bf16),
        ],
        compiler_params=PARAMS,
        name="attend",
    )(me, lengths, *blocks)


def close_kernel(
    me_ref, ret_ref, comb_ref, hid_ref, gain_ref, wdkv_ref, att_ref, next_ref, small_ref
):
    rows = comb_ref.shape[0]
    keys = wdkv_ref.shape[1]
    returned = ret_ref[...].reshape(rows, ret_ref.shape[-1])
    comb = comb_ref[...]
    high = comb.astype(bf16)
    low = (comb - high.astype(f32)).astype(bf16)
    first_dim = (((0,), (0,)), ((), ()))
    moe = lax.dot_general(
        high, returned, first_dim, preferred_element_type=f32
    ) + lax.dot_general(low, returned, first_dim, preferred_element_type=f32)
    result = (hid_ref[...].astype(f32) + moe).astype(bf16)
    next_ref[...] = result
    wide = result.astype(f32)
    square = jnp.sum(wide * wide, -1, keepdims=True)
    first = square.astype(bf16).astype(f32)
    second = (square - first).astype(bf16).astype(f32)
    third = square - first - second
    lane = lax.broadcasted_iota(jnp.int32, (wide.shape[0], small_ref.shape[2] - keys), 1)
    tail = jnp.where(
        lane == 0, first, jnp.where(lane == 1, second, jnp.where(lane == 2, third, 0.0))
    ).astype(bf16)
    down = jnp.dot(
        (wide * gain_ref[...]).astype(bf16), wdkv_ref[...], preferred_element_type=f32
    ).astype(bf16)
    tokens, peers = wide.shape[0], small_ref.shape[0]
    for j in range(peers):
        small_ref[j, :tokens, :keys] = down
        small_ref[j, :tokens, keys:] = tail
        small_ref[lax.rem(me_ref[0] + (peers - j), peers), tokens:, :] = att_ref[j]


def close(me, returned, combine, hidden, gain, w_dkv, attended):
    tokens, width = hidden.shape
    peers, extra, lanes = attended.shape
    return pl.pallas_call(
        close_kernel,
        out_shape=(
            shape((tokens, width), bf16),
            shape((peers, tokens + extra, lanes), bf16),
        ),
        in_specs=[SMEM] + [VMEM] * 6,
        out_specs=(VMEM, VMEM),
        compiler_params=PARAMS,
        name="close",
    )(me, returned, combine, hidden, gain, w_dkv, attended)


def merge_kernel(all_ref, gain_ref, cos_ref, sin_ref, q_ref, o_ref, back_ref):
    peers = all_ref.shape[0]
    seqs, heads, _ = back_ref.shape
    own = seqs // peers
    for j in range(peers):
        for i in range(own):
            at = seqs + i * heads
            back_ref[j * own + i] = all_ref[j, at : at + heads, :]
    keys = q_ref.shape[-1]
    total = all_ref[0, :seqs, :].astype(f32)
    for j in range(1, peers):
        total = total + all_ref[j, :seqs, :].astype(f32)
    square = jnp.sum(total[:, keys:], -1, keepdims=True)
    down = total[:, :keys] * lax.rsqrt(square / D + epsilon)
    latent = down[:, :LAT]
    latent = (
        latent
        * lax.rsqrt(jnp.mean(latent * latent, -1, keepdims=True) + epsilon)
        * gain_ref[...]
    )
    rope = down[:, LAT:]
    half = rope.shape[-1] // 2
    turned = jnp.concatenate([rope[:, half:], rope[:, :half]], 1)
    rope = rope * cos_ref[...] + turned * sin_ref[...]
    latent = latent.astype(bf16).astype(f32)[:, None, :]
    rope = rope.astype(bf16).astype(f32)[:, None, :]
    own = (
        jnp.sum(q_ref[:, :, :LAT].astype(f32) * latent, -1, keepdims=True)
        + jnp.sum(q_ref[:, :, LAT:].astype(f32) * rope, -1, keepdims=True)
    ) * score_scale
    cached = jnp.sum(back_ref[:, :, LAT:].astype(f32), -1, keepdims=True)
    peak = jnp.maximum(own, cached)
    own_prob = jnp.exp(own - peak)
    cached_prob = jnp.exp(cached - peak)
    total_prob = own_prob + cached_prob
    o_ref[...] = (
        back_ref[:, :, :LAT].astype(f32) * (cached_prob / total_prob)
        + latent * (own_prob / total_prob)
    ).astype(bf16)


def merge(everything, gain, cos, sin, queries):
    seqs, heads, _ = queries.shape
    return pl.pallas_call(
        merge_kernel,
        out_shape=shape((seqs, heads, LAT), bf16),
        in_specs=[VMEM] * 5,
        out_specs=VMEM,
        scratch_shapes=[pltpu.VMEM((seqs, heads, LAT + 128), bf16)],
        compiler_params=PARAMS,
        name="merge",
    )(everything, gain, cos, sin, queries)


def rope_tables(lengths, half):
    inv_freq = 10000.0 ** (-jnp.arange(half, dtype=f32) / half)
    angles = lengths.astype(f32)[:, None] * inv_freq[None, :]
    cos, sin = jnp.cos(angles), jnp.sin(angles)
    return jnp.concatenate([cos, cos], 1), jnp.concatenate([-sin, sin], 1)


def local(
    hidden,
    moe_gain,
    expert_ids,
    slots,
    affinity,
    w_gate,
    w_up,
    w_down,
    attn_gain,
    w_dkv,
    kv_gain,
    queries,
    cache,
    lengths,
):
    seqs, width = hidden.shape
    peers = lax.axis_size("tp")
    experts = lax.axis_size("ep") * lax.axis_size("mb")
    me = lax.axis_index("tp").astype(jnp.int32).reshape(1)

    def moved(x, k):
        return lax.ppermute(x, "tp", [(i, (i + k) % peers) for i in range(peers)])

    send_rows, combine = route(expert_ids, slots, affinity, hidden, experts)
    arrived = exchange(send_rows, ("ep", "mb"))
    blocks = list(pack(me, w_down[0], cache, queries, peers))
    for k in EARLY + LATE:
        blocks[k] = moved(blocks[k], k)
    parts = ring(packed_rows(arrived, moe_gain[None]), moved, peers)
    span, heads, keys = cache.shape[1], queries.shape[1], queries.shape[2]
    attended = attend(me, lengths, blocks, seqs // peers, span, heads, keys)
    units = expert_units(me, parts, w_gate[0], w_up[0], peers)
    all_units = exchange(units, "tp")
    output = expert_down(me, all_units, blocks, experts, width)
    returned = exchange(output, ("ep", "mb"))
    next_hidden, small = close(
        me, returned, combine, hidden, attn_gain[None], w_dkv, attended
    )
    everything = exchange(small, "tp")
    cos, sin = rope_tables(lengths, (keys - LAT) // 2)
    latent_out = merge(everything, kv_gain[None], cos, sin, queries)
    return (next_hidden, latent_out)


def solution(mesh):
    return jax.shard_map(
        local,
        mesh=mesh,
        in_specs=(
            P(("grp", "ep", "mb"), "tp"),
            P("tp"),
            P(("grp", "ep", "mb"), None),
            P(("grp", "ep", "mb"), None),
            P(("grp", "ep", "mb"), None),
            P(("ep", "mb"), None, "tp"),
            P(("ep", "mb"), None, "tp"),
            P(("ep", "mb"), "tp", None),
            P("tp"),
            P("tp", None),
            P(),
            P(("grp", "ep", "mb"), "tp", None),
            P(("grp", "ep", "mb"), "tp", None),
            P(("grp", "ep", "mb")),
        ),
        out_specs=(P(("grp", "ep", "mb"), "tp"), P(("grp", "ep", "mb"), "tp", None)),
        check_vma=False,
    )
```

```python
import jax
import jax.numpy as jnp
from jax import lax
from jax.experimental import pallas as pl
from jax.experimental.pallas import tpu as pltpu
from jax.sharding import PartitionSpec as P


D = 3584
LAT = 512
CAP = 8
BEFORE = (4, 3, 5)
MOVES = BEFORE + (2, 6, 1, 7)

epsilon = 1e-06
route_scale = 2.5
score_scale = 192.0 ** (-0.5)
f32 = jnp.float32
bf16 = jnp.bfloat16
VMEM = pl.BlockSpec(memory_space=pltpu.VMEM)
SMEM = pl.BlockSpec(memory_space=pltpu.SMEM)
HBM = pl.BlockSpec(memory_space=pltpu.HBM)
PARAMS = pltpu.CompilerParams(vmem_limit_bytes=40 * 1024 * 1024)


def shape(dims, dtype):
    return jax.ShapeDtypeStruct(dims, dtype)


def exchange(x, axis):
    return lax.all_to_all(x, axis, split_axis=0, concat_axis=0, tiled=True)


def in_hbm(x):
    return pltpu.with_memory_space_constraint(x, pltpu.HBM)


def fetch(sources, targets, sems):
    copies = [
        pltpu.make_async_copy(source, target, sems.at[i])
        for i, (source, target) in enumerate(zip(sources, targets))
    ]
    for copy in copies:
        copy.start()
    return copies


def route_kernel(ids_hbm, slots_hbm, aff_hbm, hid_hbm, send_ref, comb_ref, *refs):
    ids_ref, slots_ref, aff_ref, hid_ref, sems = refs
    copies = fetch((ids_hbm, slots_hbm, aff_hbm, hid_hbm), refs[:4], sems)
    for copy in copies:
        copy.wait()
    experts = send_ref.shape[0]
    top, tokens = ids_ref.shape
    rows = experts * CAP
    slots = slots_ref[...]
    affinity = aff_ref[...]
    weight = route_scale * affinity / jnp.sum(affinity, 0, keepdims=True)
    target = jnp.where(slots < CAP, ids_ref[...] * CAP + slots, -1)
    row = lax.broadcasted_iota(jnp.int32, (rows, tokens), 0)
    pick = jnp.zeros((rows, tokens), f32)
    comb = jnp.zeros((rows, tokens), f32)
    for k in range(top):
        match = target[k : k + 1, :] == row
        pick = jnp.where(match, 1.0, pick)
        comb = jnp.where(match, weight[k : k + 1, :], comb)
    comb_ref[...] = comb
    sent = jnp.dot(pick.astype(bf16), hid_ref[...], preferred_element_type=f32)
    send_ref[...] = sent.reshape(send_ref.shape).astype(bf16)


def route(expert_ids, slots, affinity, hidden, experts):
    tokens, width = hidden.shape
    inputs = (expert_ids.T, slots.T, affinity.T, hidden)
    return pl.pallas_call(
        route_kernel,
        out_shape=(shape((experts, CAP, width), bf16), shape((experts * CAP, tokens), f32)),
        in_specs=[HBM] * 4,
        out_specs=(VMEM, VMEM),
        scratch_shapes=[pltpu.VMEM(x.shape, x.dtype) for x in inputs]
        + [pltpu.SemaphoreType.DMA((4,))],
        compiler_params=PARAMS,
        name="route",
    )(*[in_hbm(x) for x in inputs])


def gain_of(block, at, width):
    rows = block[at : at + 16, :].astype(f32)
    tiles = (width + 127) // 128
    total = rows[:tiles] + rows[tiles : 2 * tiles] + rows[2 * tiles : 3 * tiles]
    return [total[q : q + 1, : min(128, width - 128 * q)] for q in range(tiles)]


def units_kernel(me_ref, wg_hbm, wu_hbm, att_ref, *refs):
    peers = att_ref.shape[0]
    blocks, parts = refs[:peers], refs[peers : 2 * peers + 1]
    o_ref, wg_ref, wu_ref, n_ref, g_ref, u_ref, sems = refs[2 * peers + 1 :]
    copies = fetch((wg_hbm, wu_hbm), (wg_ref, wu_ref), sems)
    half, double = parts[0].shape
    rows, cols, middle = 2 * half, double // 2, peers // 2
    square = jnp.zeros((rows, 1), f32)
    for k in range(peers):
        at = 0
        for part in parts[k : k + 1] if k < middle else parts[k : k + 2] if k == middle else parts[k + 1 : k + 2]:
            end = at + part.shape[0]
            n_ref[k, at:end, :] = part[:, :cols]
            n_ref[k, half + at : half + end, :] = part[:, cols:]
            at = end
        x = n_ref[k].astype(f32)
        square = square + jnp.sum(x * x, -1, keepdims=True)
    scale = lax.rsqrt(square / D + epsilon)
    copies[0].wait()
    copies[1].wait()
    for k in range(peers):
        j = lax.rem(me_ref[0] + (peers - k), peers)
        gain = jnp.concatenate(gain_of(blocks[k], blocks[k].shape[0] - 16, cols), 1)
        normed = (n_ref[k].astype(f32) * scale * gain).astype(bf16)
        part = pl.ds(pl.multiple_of(j * cols, 64), cols)
        gate = jnp.dot(normed, wg_ref[part, :], preferred_element_type=f32)
        up = jnp.dot(normed, wu_ref[part, :], preferred_element_type=f32)
        if k == 0:
            g_ref[...] = gate
            u_ref[...] = up
        else:
            g_ref[...] += gate
            u_ref[...] += up
        o_ref[j, rows:, :] = att_ref[k]
    gate = g_ref[...]
    units = (gate / (1.0 + jnp.exp(-gate)) * u_ref[...]).astype(bf16)
    for j in range(peers):
        o_ref[j, :rows, :] = units


def expert_units(me, parts, w_gate, w_up, attended, blocks):
    peers = len(blocks)
    half, double = parts[0].shape
    rows, cols, hid = 2 * half, double // 2, w_gate.shape[1]
    return pl.pallas_call(
        units_kernel,
        out_shape=shape((peers, rows + attended.shape[1], hid), bf16),
        in_specs=[SMEM, HBM, HBM] + [VMEM] * (2 * peers + 2),
        out_specs=VMEM,
        scratch_shapes=[
            pltpu.VMEM(w_gate.shape, bf16),
            pltpu.VMEM(w_up.shape, bf16),
            pltpu.VMEM((peers, rows, cols), bf16),
            pltpu.VMEM((rows, hid), f32),
            pltpu.VMEM((rows, hid), f32),
            pltpu.SemaphoreType.DMA((2,)),
        ],
        compiler_params=PARAMS,
        name="units",
    )(me, in_hbm(w_gate), in_hbm(w_up), attended, *blocks, *parts)


def pack_kernel(me_ref, wd_hbm, cache_hbm, q_hbm, gain_hbm, *refs):
    outs, (wd_ref, cache_ref, q_ref, gain_ref, tiles_ref, keys_ref, sems) = refs[:-7], refs[-7:]
    copies = fetch(
        (wd_hbm, cache_hbm, q_hbm, gain_hbm), (wd_ref, cache_ref, q_ref, gain_ref), sems
    )
    peers = len(outs)
    half, double = tiles_ref.shape[1:]
    width = double // 2
    span, heads, keys = cache_ref.shape[1], q_ref.shape[1], cache_ref.shape[2]
    own = cache_ref.shape[0] // peers
    copies[0].wait()
    for j in range(peers):
        tiles_ref[j, :, :width] = wd_ref[:half, j * width : (j + 1) * width]
        tiles_ref[j, :, width:] = wd_ref[half:, j * width : (j + 1) * width]
    copies[3].wait()
    gain = gain_ref[...]
    first = gain.astype(bf16).astype(f32)
    second = (gain - first).astype(bf16).astype(f32)
    row = lax.broadcasted_iota(jnp.int32, (16, 128), 0)
    packed = jnp.zeros((16, 128), f32)
    tiles = (width + 127) // 128
    for p, value in enumerate((first, second, gain - first - second)):
        for q in range(tiles):
            piece = value[:, 128 * q : min(128 * (q + 1), width)]
            if piece.shape[1] < 128:
                piece = jnp.concatenate([piece, jnp.zeros((1, 128 - piece.shape[1]), f32)], 1)
            packed = jnp.where(row == p * tiles + q, piece, packed)
    packed = packed.astype(bf16)
    copies[1].wait()
    copies[2].wait()
    for k in range(peers):
        to = lax.rem(me_ref[0] + k, peers)
        at = 0
        for t in range(double // 128):
            outs[k][at : at + half, :] = tiles_ref[to, :, 128 * t : 128 * (t + 1)]
            at += half
        for i in range(own):
            keys_ref[:span, i * keys : (i + 1) * keys] = cache_ref[to * own + i]
            keys_ref[span:, i * keys : (i + 1) * keys] = q_ref[to * own + i]
        for t in range(own * keys // 128):
            outs[k][at : at + span + heads, :] = keys_ref[:, 128 * t : 128 * (t + 1)]
            at += span + heads
        outs[k][at : at + 16, :] = packed


def pack(me, w_down, cache, queries, gain, peers):
    hid, width = w_down.shape[0], w_down.shape[1] // peers
    seqs, span, keys = cache.shape
    own, heads = seqs // peers, queries.shape[1]
    rows = hid * width // 128 + own * (span + heads) * keys // 128 + 16
    return pl.pallas_call(
        pack_kernel,
        out_shape=tuple(shape((rows, 128), bf16) for _ in range(peers)),
        in_specs=[SMEM] + [HBM] * 4,
        out_specs=tuple(VMEM for _ in range(peers)),
        scratch_shapes=[
            pltpu.VMEM(w_down.shape, bf16),
            pltpu.VMEM(cache.shape, bf16),
            pltpu.VMEM(queries.shape, bf16),
            pltpu.VMEM(gain.shape, f32),
            pltpu.VMEM((peers, hid // 2, 2 * width), bf16),
            pltpu.VMEM((span + heads, own * keys), bf16),
            pltpu.SemaphoreType.DMA((4,)),
        ],
        compiler_params=PARAMS,
        name="pack",
    )(me, in_hbm(w_down), in_hbm(cache), in_hbm(queries), in_hbm(gain))


def rows_kernel(x_ref, o_ref):
    half, double = o_ref.shape
    width = double // 2
    x = x_ref[...].reshape(2 * half, width)
    o_ref[:, :width] = x[:half]
    o_ref[:, width:] = x[half:]


def packed_rows(arrived):
    experts, cap, width = arrived.shape
    return pl.pallas_call(
        rows_kernel,
        out_shape=shape((experts * cap // 2, 2 * width), bf16),
        in_specs=[VMEM],
        out_specs=VMEM,
        compiler_params=PARAMS,
        name="rows",
    )(arrived)


def ring(x, moved, peers):
    steps, half = peers // 2, x.shape[0] // 2
    there, back = [x], [x]
    for _ in range(1, steps):
        there.append(moved(there[-1], 1))
        back.append(moved(back[-1], peers - 1))
    upper = moved(there[-1][:half], 1)
    lower = moved(back[-1][half:], peers - 1)
    return there + [upper, lower] + back[:0:-1]


def columns_kernel(*refs):
    blocks, o_ref, w_ref = refs[:-2], refs[-2], refs[-1]
    half, double = w_ref.shape
    width = double // 2
    for k in range(len(blocks)):
        for t in range(double // 128):
            w_ref[:, 128 * t : 128 * (t + 1)] = blocks[k][half * t : half * (t + 1), :]
        o_ref[k, :half, :] = w_ref[:, :width]
        o_ref[k, half:, :] = w_ref[:, width:]


def columns_of(blocks, hid, width):
    return pl.pallas_call(
        columns_kernel,
        out_shape=shape((len(blocks), hid, width), bf16),
        in_specs=[VMEM] * len(blocks),
        out_specs=VMEM,
        scratch_shapes=[pltpu.VMEM((hid // 2, 2 * width), bf16)],
        compiler_params=PARAMS,
        name="columns",
    )(*blocks)


def down_kernel(me_ref, u_ref, w_ref, o_ref):
    peers = u_ref.shape[0]
    experts, cap, width = o_ref.shape
    acc = jnp.zeros((experts * cap, width), f32)
    for k in range(peers):
        group = lax.rem(me_ref[0] + (peers - k), peers)
        acc = acc + jnp.dot(
            u_ref[group, : experts * cap, :], w_ref[k], preferred_element_type=f32
        )
    o_ref[...] = acc.reshape(o_ref.shape).astype(bf16)


def expert_down(me, units, columns, experts):
    return pl.pallas_call(
        down_kernel,
        out_shape=shape((experts, CAP, columns.shape[2]), bf16),
        in_specs=[SMEM, VMEM, VMEM],
        out_specs=VMEM,
        compiler_params=PARAMS,
        name="down",
    )(me, units, columns)


def attend_kernel(me_ref, len_ref, *refs):
    peers = len(refs) - 4
    blocks, (o_ref, m_ref, c_ref, q_ref) = refs[:peers], refs[peers:]
    own, positions, keys = c_ref.shape
    span, heads = positions // peers, q_ref.shape[1] // peers
    me = me_ref[0]
    first = blocks[0].shape[0] - 16 - own * keys // 128 * (span + heads)
    for k in range(peers):
        for t in range(own * keys // 128):
            at = first + t * (span + heads)
            m_ref[:, 128 * t : 128 * (t + 1)] = blocks[k][at : at + span + heads, :]
        for i in range(own):
            c_ref[i, k * span : (k + 1) * span, :] = m_ref[:span, i * keys : (i + 1) * keys]
            q_ref[i, k * heads : (k + 1) * heads, :] = m_ref[span:, i * keys : (i + 1) * keys]
    lane = lax.broadcasted_iota(jnp.int32, (peers * heads, positions), 1)
    block = lax.rem(me + (peers - lane // span), peers)
    position = block * span + lane % span
    for i in range(own):
        live = position < len_ref[me * own + i]
        known = c_ref[i]
        scores = (
            lax.dot_general(
                q_ref[i], known, (((1,), (1,)), ((), ())), preferred_element_type=f32
            )
            * score_scale
        )
        scores = jnp.where(live, scores, -1e30)
        peak = jnp.max(scores, -1, keepdims=True)
        prob = jnp.where(live, jnp.exp(scores - peak), 0.0)
        mass = jnp.sum(prob, -1, keepdims=True)
        out = jnp.dot(prob.astype(bf16), known[:, :LAT], preferred_element_type=f32)
        out = (out / mass).astype(bf16)
        total = peak + jnp.log(mass)
        high = total.astype(bf16).astype(f32)
        middle = (total - high).astype(bf16).astype(f32)
        low = total - high - middle
        tail_lane = lax.broadcasted_iota(jnp.int32, (peers * heads, 128), 1)
        tail = jnp.where(
            tail_lane == 0,
            high,
            jnp.where(tail_lane == 1, middle, jnp.where(tail_lane == 2, low, 0.0)),
        ).astype(bf16)
        for k in range(peers):
            for t in range(LAT // 128 + 1):
                at = (t * own + i) * heads
                piece = tail if t == LAT // 128 else out[:, 128 * t : 128 * (t + 1)]
                o_ref[k, at : at + heads, :] = piece[k * heads : (k + 1) * heads]


def attend(me, lengths, blocks, own, span, heads, keys):
    peers = len(blocks)
    return pl.pallas_call(
        attend_kernel,
        out_shape=shape((peers, own * heads * (LAT // 128 + 1), 128), bf16),
        in_specs=[SMEM, SMEM] + [VMEM] * peers,
        out_specs=VMEM,
        scratch_shapes=[
            pltpu.VMEM((span + heads, own * keys), bf16),
            pltpu.VMEM((own, peers * span, keys), bf16),
            pltpu.VMEM((own, peers * heads, keys), bf16),
        ],
        compiler_params=PARAMS,
        name="attend",
    )(me, lengths, *blocks)


def close_kernel(ret_ref, comb_ref, hid_ref, gain_ref, wdkv_ref, next_ref, small_ref):
    rows = comb_ref.shape[0]
    keys = wdkv_ref.shape[1]
    returned = ret_ref[...].reshape(rows, ret_ref.shape[-1])
    comb = comb_ref[...]
    high = comb.astype(bf16)
    low = (comb - high.astype(f32)).astype(bf16)
    first_dim = (((0,), (0,)), ((), ()))
    moe = lax.dot_general(
        high, returned, first_dim, preferred_element_type=f32
    ) + lax.dot_general(low, returned, first_dim, preferred_element_type=f32)
    result = (hid_ref[...].astype(f32) + moe).astype(bf16)
    next_ref[...] = result
    wide = result.astype(f32)
    square = jnp.sum(wide * wide, -1, keepdims=True)
    first = square.astype(bf16).astype(f32)
    second = (square - first).astype(bf16).astype(f32)
    third = square - first - second
    lane = lax.broadcasted_iota(jnp.int32, (wide.shape[0], small_ref.shape[2] - keys), 1)
    tail = jnp.where(
        lane == 0, first, jnp.where(lane == 1, second, jnp.where(lane == 2, third, 0.0))
    ).astype(bf16)
    down = jnp.dot(
        (wide * gain_ref[...]).astype(bf16), wdkv_ref[...], preferred_element_type=f32
    ).astype(bf16)
    for j in range(small_ref.shape[0]):
        small_ref[j, :, :keys] = down
        small_ref[j, :, keys:] = tail


def close(returned, combine, hidden, gain, w_dkv, peers):
    tokens, width = hidden.shape
    return pl.pallas_call(
        close_kernel,
        out_shape=(
            shape((tokens, width), bf16),
            shape((peers, tokens, w_dkv.shape[1] + 64), bf16),
        ),
        in_specs=[VMEM] * 5,
        out_specs=(VMEM, VMEM),
        compiler_params=PARAMS,
        name="close",
    )(returned, combine, hidden, gain, w_dkv)


def merge_kernel(all_ref, table_ref, q_ref, units_ref, o_ref, back_ref):
    peers = all_ref.shape[0]
    seqs, heads, lanes = back_ref.shape
    own = seqs // peers
    first = units_ref.shape[1] - own * heads * (lanes // 128)
    for j in range(peers):
        for i in range(own):
            for t in range(lanes // 128):
                at = first + (t * own + i) * heads
                back_ref[j * own + i, :, 128 * t : 128 * (t + 1)] = units_ref[
                    j, at : at + heads, :
                ]
    keys = q_ref.shape[-1]
    total = all_ref[0].astype(f32)
    for j in range(1, all_ref.shape[0]):
        total = total + all_ref[j].astype(f32)
    square = jnp.sum(total[:, keys:], -1, keepdims=True)
    down = total[:, :keys] * lax.rsqrt(square / D + epsilon)
    latent = down[:, :LAT]
    latent = (
        latent
        * lax.rsqrt(jnp.mean(latent * latent, -1, keepdims=True) + epsilon)
        * table_ref[:1, :LAT]
    )
    rope = down[:, LAT:]
    half = rope.shape[-1] // 2
    turned = jnp.concatenate([rope[:, half:], rope[:, :half]], 1)
    cos, sin = LAT + 2 * half, LAT + 4 * half
    rope = rope * table_ref[:, LAT:cos] + turned * table_ref[:, cos:sin]
    latent = latent.astype(bf16).astype(f32)[:, None, :]
    rope = rope.astype(bf16).astype(f32)[:, None, :]
    own = (
        jnp.sum(q_ref[:, :, :LAT].astype(f32) * latent, -1, keepdims=True)
        + jnp.sum(q_ref[:, :, LAT:].astype(f32) * rope, -1, keepdims=True)
    ) * score_scale
    cached = jnp.sum(back_ref[:, :, LAT:].astype(f32), -1, keepdims=True)
    peak = jnp.maximum(own, cached)
    own_prob = jnp.exp(own - peak)
    cached_prob = jnp.exp(cached - peak)
    total_prob = own_prob + cached_prob
    o_ref[...] = (
        back_ref[:, :, :LAT].astype(f32) * (cached_prob / total_prob)
        + latent * (own_prob / total_prob)
    ).astype(bf16)


def merge(everything, table, queries, units):
    seqs, heads, _ = queries.shape
    return pl.pallas_call(
        merge_kernel,
        out_shape=shape((seqs, heads, LAT), bf16),
        in_specs=[VMEM] * 4,
        out_specs=VMEM,
        scratch_shapes=[pltpu.VMEM((seqs, heads, LAT + 128), bf16)],
        compiler_params=PARAMS,
        name="merge",
    )(everything, table, queries, units)


def rope_tables(lengths, half):
    inv_freq = 10000.0 ** (-jnp.arange(half, dtype=f32) / half)
    angles = lengths.astype(f32)[:, None] * inv_freq[None, :]
    cos, sin = jnp.cos(angles), jnp.sin(angles)
    return jnp.concatenate([cos, cos], 1), jnp.concatenate([-sin, sin], 1)


def local(
    hidden,
    moe_gain,
    expert_ids,
    slots,
    affinity,
    w_gate,
    w_up,
    w_down,
    attn_gain,
    w_dkv,
    kv_gain,
    queries,
    cache,
    lengths,
):
    seqs, width = hidden.shape
    peers = lax.axis_size("tp")
    experts = lax.axis_size("ep") * lax.axis_size("mb")
    me = lax.axis_index("tp").astype(jnp.int32).reshape(1)

    def moved(x, k):
        return lax.ppermute(x, "tp", [(i, (i + k) % peers) for i in range(peers)])

    send_rows, combine = route(expert_ids, slots, affinity, hidden, experts)
    arrived = exchange(send_rows, ("ep", "mb"))
    blocks = list(pack(me, w_down[0], cache, queries, moe_gain[None], peers))
    for k in MOVES:
        blocks[k] = moved(blocks[k], k)
    parts = ring(packed_rows(arrived), moved, peers)
    span, heads, keys = cache.shape[1], queries.shape[1], queries.shape[2]
    attended = attend(me, lengths, blocks, seqs // peers, span, heads, keys)
    units = expert_units(me, parts, w_gate[0], w_up[0], attended, blocks)
    all_units = exchange(units, "tp")
    columns = columns_of(blocks, w_down.shape[1], width)
    output = expert_down(me, all_units, columns, experts)
    returned = exchange(output, ("ep", "mb"))
    next_hidden, small = close(returned, combine, hidden, attn_gain[None], w_dkv, peers)
    everything = exchange(small, "tp")
    gain = jnp.broadcast_to(kv_gain, (seqs, LAT))
    table = jnp.concatenate([gain, *rope_tables(lengths, (keys - LAT) // 2)], 1)
    latent_out = merge(everything, table, queries, all_units)
    return (next_hidden, latent_out)


def solution(mesh):
    return jax.shard_map(
        local,
        mesh=mesh,
        in_specs=(
            P(("grp", "ep", "mb"), "tp"),
            P("tp"),
            P(("grp", "ep", "mb"), None),
            P(("grp", "ep", "mb"), None),
            P(("grp", "ep", "mb"), None),
            P(("ep", "mb"), None, "tp"),
            P(("ep", "mb"), None, "tp"),
            P(("ep", "mb"), "tp", None),
            P("tp"),
            P("tp", None),
            P(),
            P(("grp", "ep", "mb"), "tp", None),
            P(("grp", "ep", "mb"), "tp", None),
            P(("grp", "ep", "mb")),
        ),
        out_specs=(P(("grp", "ep", "mb"), "tp"), P(("grp", "ep", "mb"), "tp", None)),
        check_vma=False,
    )
```

```python
import jax
import jax.numpy as jnp
from jax import lax
from jax.experimental import pallas as pl
from jax.experimental.pallas import tpu as pltpu
from jax.sharding import PartitionSpec as P


D = 3584
LAT = 512
CAP = 8
BEFORE = (4, 3, 5)
MOVES = BEFORE + (2, 6, 1, 7)

epsilon = 1e-06
route_scale = 2.5
score_scale = 192.0 ** (-0.5)
f32 = jnp.float32
bf16 = jnp.bfloat16
VMEM = pl.BlockSpec(memory_space=pltpu.VMEM)
SMEM = pl.BlockSpec(memory_space=pltpu.SMEM)
HBM = pl.BlockSpec(memory_space=pltpu.HBM)
PARAMS = pltpu.CompilerParams(vmem_limit_bytes=40 * 1024 * 1024)


def shape(dims, dtype):
    return jax.ShapeDtypeStruct(dims, dtype)


def exchange(x, axis):
    return lax.all_to_all(x, axis, split_axis=0, concat_axis=0, tiled=True)


def in_hbm(x):
    return pltpu.with_memory_space_constraint(x, pltpu.HBM)


def fetch(sources, targets, sems):
    copies = [
        pltpu.make_async_copy(source, target, sems.at[i])
        for i, (source, target) in enumerate(zip(sources, targets))
    ]
    for copy in copies:
        copy.start()
    return copies


def route_kernel(ids_hbm, slots_hbm, aff_hbm, hid_hbm, send_ref, comb_ref, *refs):
    ids_ref, slots_ref, aff_ref, hid_ref, sems = refs
    copies = fetch((ids_hbm, slots_hbm, aff_hbm, hid_hbm), refs[:4], sems)
    for copy in copies:
        copy.wait()
    experts = send_ref.shape[0]
    top, tokens = ids_ref.shape
    rows = experts * CAP
    slots = slots_ref[...]
    affinity = aff_ref[...]
    weight = route_scale * affinity / jnp.sum(affinity, 0, keepdims=True)
    target = jnp.where(slots < CAP, ids_ref[...] * CAP + slots, -1)
    row = lax.broadcasted_iota(jnp.int32, (rows, tokens), 0)
    pick = jnp.zeros((rows, tokens), f32)
    comb = jnp.zeros((rows, tokens), f32)
    for k in range(top):
        match = target[k : k + 1, :] == row
        pick = jnp.where(match, 1.0, pick)
        comb = jnp.where(match, weight[k : k + 1, :], comb)
    comb_ref[...] = comb
    sent = jnp.dot(pick.astype(bf16), hid_ref[...], preferred_element_type=f32)
    send_ref[...] = sent.reshape(send_ref.shape).astype(bf16)


def route(expert_ids, slots, affinity, hidden, experts):
    tokens, width = hidden.shape
    inputs = (expert_ids.T, slots.T, affinity.T, hidden)
    return pl.pallas_call(
        route_kernel,
        out_shape=(shape((experts, CAP, width), bf16), shape((experts * CAP, tokens), f32)),
        in_specs=[HBM] * 4,
        out_specs=(VMEM, VMEM),
        scratch_shapes=[pltpu.VMEM(x.shape, x.dtype) for x in inputs]
        + [pltpu.SemaphoreType.DMA((4,))],
        compiler_params=PARAMS,
        name="route",
    )(*[in_hbm(x) for x in inputs])


def gain_of(block, at, width):
    rows = block[at : at + 16, :].astype(f32)
    tiles = (width + 127) // 128
    total = rows[:tiles] + rows[tiles : 2 * tiles] + rows[2 * tiles : 3 * tiles]
    return [total[q : q + 1, : min(128, width - 128 * q)] for q in range(tiles)]


def units_kernel(me_ref, wg_hbm, wu_hbm, att_ref, *refs):
    peers = att_ref.shape[0]
    blocks, parts = refs[:peers], refs[peers : 2 * peers + 1]
    o_ref, wg_ref, wu_ref, n_ref, g_ref, u_ref, sems = refs[2 * peers + 1 :]
    copies = fetch((wg_hbm, wu_hbm), (wg_ref, wu_ref), sems)
    _, rows, cols = n_ref.shape
    middle, tiles = peers // 2, cols // 128
    square = jnp.zeros((rows, 1), f32)
    for k in range(peers):
        at = 0
        first = k if k <= middle else k + 1
        for part in parts[first : first + (2 if k == middle else 1)]:
            done = 0
            while done < part.shape[0]:
                tile, row = divmod(at, rows)
                take = min(part.shape[0] - done, (rows if tile < tiles else rows // 2) - row)
                piece = part[done : done + take, :]
                if tile < tiles:
                    n_ref[k, row : row + take, 128 * tile : 128 * (tile + 1)] = piece
                else:
                    n_ref[k, row : row + take, 128 * tiles :] = piece[:, :64]
                    n_ref[k, rows // 2 + row : rows // 2 + row + take, 128 * tiles :] = piece[:, 64:]
                at, done = at + take, done + take
        x = n_ref[k].astype(f32)
        square = square + jnp.sum(x * x, -1, keepdims=True)
    scale = lax.rsqrt(square / D + epsilon)
    copies[0].wait()
    copies[1].wait()
    for k in range(peers):
        j = lax.rem(me_ref[0] + (peers - k), peers)
        gain = jnp.concatenate(gain_of(blocks[k], blocks[k].shape[0] - 16, cols), 1)
        normed = (n_ref[k].astype(f32) * scale * gain).astype(bf16)
        part = pl.ds(pl.multiple_of(j * cols, 64), cols)
        gate = jnp.dot(normed, wg_ref[part, :], preferred_element_type=f32)
        up = jnp.dot(normed, wu_ref[part, :], preferred_element_type=f32)
        if k == 0:
            g_ref[...] = gate
            u_ref[...] = up
        else:
            g_ref[...] += gate
            u_ref[...] += up
        o_ref[j, rows:, :] = att_ref[k]
    gate = g_ref[...]
    units = (gate / (1.0 + jnp.exp(-gate)) * u_ref[...]).astype(bf16)
    for j in range(peers):
        o_ref[j, :rows, :] = units


def expert_units(me, parts, w_gate, w_up, attended, blocks):
    peers = len(blocks)
    cols, hid = w_gate.shape[0] // peers, w_gate.shape[1]
    rows = parts[0].shape[0] * 128 // cols
    return pl.pallas_call(
        units_kernel,
        out_shape=shape((peers, rows + attended.shape[1], hid), bf16),
        in_specs=[SMEM, HBM, HBM] + [VMEM] * (2 * peers + 2),
        out_specs=VMEM,
        scratch_shapes=[
            pltpu.VMEM(w_gate.shape, bf16),
            pltpu.VMEM(w_up.shape, bf16),
            pltpu.VMEM((peers, rows, cols), bf16),
            pltpu.VMEM((rows, hid), f32),
            pltpu.VMEM((rows, hid), f32),
            pltpu.SemaphoreType.DMA((2,)),
        ],
        compiler_params=PARAMS,
        name="units",
    )(me, in_hbm(w_gate), in_hbm(w_up), attended, *blocks, *parts)


def pack_kernel(me_ref, wd_hbm, cache_hbm, q_hbm, gain_hbm, *refs):
    outs, (wd_ref, cache_ref, q_ref, gain_ref, tiles_ref, keys_ref, sems) = refs[:-7], refs[-7:]
    copies = fetch(
        (wd_hbm, cache_hbm, q_hbm, gain_hbm), (wd_ref, cache_ref, q_ref, gain_ref), sems
    )
    peers = len(outs)
    half, double = tiles_ref.shape[1:]
    width = double // 2
    span, heads, keys = cache_ref.shape[1], q_ref.shape[1], cache_ref.shape[2]
    own = cache_ref.shape[0] // peers
    copies[0].wait()
    for j in range(peers):
        tiles_ref[j, :, :width] = wd_ref[:half, j * width : (j + 1) * width]
        tiles_ref[j, :, width:] = wd_ref[half:, j * width : (j + 1) * width]
    copies[3].wait()
    gain = gain_ref[...]
    first = gain.astype(bf16).astype(f32)
    second = (gain - first).astype(bf16).astype(f32)
    row = lax.broadcasted_iota(jnp.int32, (16, 128), 0)
    packed = jnp.zeros((16, 128), f32)
    tiles = (width + 127) // 128
    for p, value in enumerate((first, second, gain - first - second)):
        for q in range(tiles):
            piece = value[:, 128 * q : min(128 * (q + 1), width)]
            if piece.shape[1] < 128:
                piece = jnp.concatenate([piece, jnp.zeros((1, 128 - piece.shape[1]), f32)], 1)
            packed = jnp.where(row == p * tiles + q, piece, packed)
    packed = packed.astype(bf16)
    copies[1].wait()
    copies[2].wait()
    for k in range(peers):
        to = lax.rem(me_ref[0] + k, peers)
        at = 0
        for t in range(double // 128):
            outs[k][at : at + half, :] = tiles_ref[to, :, 128 * t : 128 * (t + 1)]
            at += half
        for i in range(own):
            keys_ref[:span, i * keys : (i + 1) * keys] = cache_ref[to * own + i]
            keys_ref[span:, i * keys : (i + 1) * keys] = q_ref[to * own + i]
        for t in range(own * keys // 128):
            outs[k][at : at + span + heads, :] = keys_ref[:, 128 * t : 128 * (t + 1)]
            at += span + heads
        outs[k][at : at + 16, :] = packed


def pack(me, w_down, cache, queries, gain, peers):
    hid, width = w_down.shape[0], w_down.shape[1] // peers
    seqs, span, keys = cache.shape
    own, heads = seqs // peers, queries.shape[1]
    rows = hid * width // 128 + own * (span + heads) * keys // 128 + 16
    return pl.pallas_call(
        pack_kernel,
        out_shape=tuple(shape((rows, 128), bf16) for _ in range(peers)),
        in_specs=[SMEM] + [HBM] * 4,
        out_specs=tuple(VMEM for _ in range(peers)),
        scratch_shapes=[
            pltpu.VMEM(w_down.shape, bf16),
            pltpu.VMEM(cache.shape, bf16),
            pltpu.VMEM(queries.shape, bf16),
            pltpu.VMEM(gain.shape, f32),
            pltpu.VMEM((peers, hid // 2, 2 * width), bf16),
            pltpu.VMEM((span + heads, own * keys), bf16),
            pltpu.SemaphoreType.DMA((4,)),
        ],
        compiler_params=PARAMS,
        name="pack",
    )(me, in_hbm(w_down), in_hbm(cache), in_hbm(queries), in_hbm(gain))


def rows_kernel(x_ref, o_ref):
    experts, cap, width = x_ref.shape
    rows = experts * cap
    x = x_ref[...].reshape(rows, width)
    tiles = width // 128
    for t in range(tiles):
        o_ref[t * rows : (t + 1) * rows, :] = x[:, 128 * t : 128 * (t + 1)]
    o_ref[tiles * rows :, :64] = x[: rows // 2, 128 * tiles :]
    o_ref[tiles * rows :, 64:] = x[rows // 2 :, 128 * tiles :]


def packed_rows(arrived):
    experts, cap, width = arrived.shape
    return pl.pallas_call(
        rows_kernel,
        out_shape=shape((experts * cap * width // 128, 128), bf16),
        in_specs=[VMEM],
        out_specs=VMEM,
        compiler_params=PARAMS,
        name="rows",
    )(arrived)


def ring(x, moved, peers):
    steps, half = peers // 2, x.shape[0] // 2
    there, back = [x], [x]
    for _ in range(1, steps):
        there.append(moved(there[-1], 1))
        back.append(moved(back[-1], peers - 1))
    upper = moved(there[-1][:half], 1)
    lower = moved(back[-1][half:], peers - 1)
    return there + [upper, lower] + back[:0:-1]


def columns_kernel(*refs):
    blocks, o_ref, w_ref = refs[:-2], refs[-2], refs[-1]
    half, double = w_ref.shape
    width = double // 2
    for k in range(len(blocks)):
        for t in range(double // 128):
            w_ref[:, 128 * t : 128 * (t + 1)] = blocks[k][half * t : half * (t + 1), :]
        o_ref[k, :half, :] = w_ref[:, :width]
        o_ref[k, half:, :] = w_ref[:, width:]


def columns_of(blocks, hid, width):
    return pl.pallas_call(
        columns_kernel,
        out_shape=shape((len(blocks), hid, width), bf16),
        in_specs=[VMEM] * len(blocks),
        out_specs=VMEM,
        scratch_shapes=[pltpu.VMEM((hid // 2, 2 * width), bf16)],
        compiler_params=PARAMS,
        name="columns",
    )(*blocks)


def down_kernel(me_ref, u_ref, w_ref, o_ref):
    peers = u_ref.shape[0]
    experts, cap, width = o_ref.shape
    acc = jnp.zeros((experts * cap, width), f32)
    for k in range(peers):
        group = lax.rem(me_ref[0] + (peers - k), peers)
        acc = acc + jnp.dot(
            u_ref[group, : experts * cap, :], w_ref[k], preferred_element_type=f32
        )
    o_ref[...] = acc.reshape(o_ref.shape).astype(bf16)


def expert_down(me, units, columns, experts):
    return pl.pallas_call(
        down_kernel,
        out_shape=shape((experts, CAP, columns.shape[2]), bf16),
        in_specs=[SMEM, VMEM, VMEM],
        out_specs=VMEM,
        compiler_params=PARAMS,
        name="down",
    )(me, units, columns)


def attend_kernel(me_ref, len_ref, *refs):
    peers = len(refs) - 4
    blocks, (o_ref, m_ref, c_ref, q_ref) = refs[:peers], refs[peers:]
    own, positions, keys = c_ref.shape
    span, heads = positions // peers, q_ref.shape[1] // peers
    me = me_ref[0]
    first = blocks[0].shape[0] - 16 - own * keys // 128 * (span + heads)
    for k in range(peers):
        for t in range(own * keys // 128):
            at = first + t * (span + heads)
            m_ref[:, 128 * t : 128 * (t + 1)] = blocks[k][at : at + span + heads, :]
        for i in range(own):
            c_ref[i, k * span : (k + 1) * span, :] = m_ref[:span, i * keys : (i + 1) * keys]
            q_ref[i, k * heads : (k + 1) * heads, :] = m_ref[span:, i * keys : (i + 1) * keys]
    lane = lax.broadcasted_iota(jnp.int32, (peers * heads, positions), 1)
    block = lax.rem(me + (peers - lane // span), peers)
    position = block * span + lane % span
    for i in range(own):
        live = position < len_ref[me * own + i]
        known = c_ref[i]
        scores = (
            lax.dot_general(
                q_ref[i], known, (((1,), (1,)), ((), ())), preferred_element_type=f32
            )
            * score_scale
        )
        scores = jnp.where(live, scores, -1e30)
        peak = jnp.max(scores, -1, keepdims=True)
        prob = jnp.where(live, jnp.exp(scores - peak), 0.0)
        mass = jnp.sum(prob, -1, keepdims=True)
        out = jnp.dot(prob.astype(bf16), known[:, :LAT], preferred_element_type=f32)
        out = (out / mass).astype(bf16)
        total = peak + jnp.log(mass)
        high = total.astype(bf16).astype(f32)
        middle = (total - high).astype(bf16).astype(f32)
        low = total - high - middle
        tail_lane = lax.broadcasted_iota(jnp.int32, (peers * heads, 128), 1)
        tail = jnp.where(
            tail_lane == 0,
            high,
            jnp.where(tail_lane == 1, middle, jnp.where(tail_lane == 2, low, 0.0)),
        ).astype(bf16)
        for k in range(peers):
            for t in range(LAT // 128 + 1):
                at = (t * own + i) * heads
                piece = tail if t == LAT // 128 else out[:, 128 * t : 128 * (t + 1)]
                o_ref[k, at : at + heads, :] = piece[k * heads : (k + 1) * heads]


def attend(me, lengths, blocks, own, span, heads, keys):
    peers = len(blocks)
    return pl.pallas_call(
        attend_kernel,
        out_shape=shape((peers, own * heads * (LAT // 128 + 1), 128), bf16),
        in_specs=[SMEM, SMEM] + [VMEM] * peers,
        out_specs=VMEM,
        scratch_shapes=[
            pltpu.VMEM((span + heads, own * keys), bf16),
            pltpu.VMEM((own, peers * span, keys), bf16),
            pltpu.VMEM((own, peers * heads, keys), bf16),
        ],
        compiler_params=PARAMS,
        name="attend",
    )(me, lengths, *blocks)


def close_kernel(ret_ref, comb_ref, hid_ref, gain_ref, wdkv_ref, next_ref, small_ref):
    rows = comb_ref.shape[0]
    keys = wdkv_ref.shape[1]
    returned = ret_ref[...].reshape(rows, ret_ref.shape[-1])
    comb = comb_ref[...]
    high = comb.astype(bf16)
    low = (comb - high.astype(f32)).astype(bf16)
    first_dim = (((0,), (0,)), ((), ()))
    moe = lax.dot_general(
        high, returned, first_dim, preferred_element_type=f32
    ) + lax.dot_general(low, returned, first_dim, preferred_element_type=f32)
    result = (hid_ref[...].astype(f32) + moe).astype(bf16)
    next_ref[...] = result
    wide = result.astype(f32)
    square = jnp.sum(wide * wide, -1, keepdims=True)
    first = square.astype(bf16).astype(f32)
    second = (square - first).astype(bf16).astype(f32)
    third = square - first - second
    lane = lax.broadcasted_iota(jnp.int32, (wide.shape[0], small_ref.shape[2] - keys), 1)
    tail = jnp.where(
        lane == 0, first, jnp.where(lane == 1, second, jnp.where(lane == 2, third, 0.0))
    ).astype(bf16)
    down = jnp.dot(
        (wide * gain_ref[...]).astype(bf16), wdkv_ref[...], preferred_element_type=f32
    ).astype(bf16)
    for j in range(small_ref.shape[0]):
        small_ref[j, :, :keys] = down
        small_ref[j, :, keys:] = tail


def close(returned, combine, hidden, gain, w_dkv, peers):
    tokens, width = hidden.shape
    return pl.pallas_call(
        close_kernel,
        out_shape=(
            shape((tokens, width), bf16),
            shape((peers, tokens, w_dkv.shape[1] + 64), bf16),
        ),
        in_specs=[VMEM] * 5,
        out_specs=(VMEM, VMEM),
        compiler_params=PARAMS,
        name="close",
    )(returned, combine, hidden, gain, w_dkv)


def merge_kernel(all_ref, table_ref, q_ref, units_ref, o_ref, back_ref):
    peers = all_ref.shape[0]
    seqs, heads, lanes = back_ref.shape
    own = seqs // peers
    first = units_ref.shape[1] - own * heads * (lanes // 128)
    for j in range(peers):
        for i in range(own):
            for t in range(lanes // 128):
                at = first + (t * own + i) * heads
                back_ref[j * own + i, :, 128 * t : 128 * (t + 1)] = units_ref[
                    j, at : at + heads, :
                ]
    keys = q_ref.shape[-1]
    total = all_ref[0].astype(f32)
    for j in range(1, all_ref.shape[0]):
        total = total + all_ref[j].astype(f32)
    square = jnp.sum(total[:, keys:], -1, keepdims=True)
    down = total[:, :keys] * lax.rsqrt(square / D + epsilon)
    latent = down[:, :LAT]
    latent = (
        latent
        * lax.rsqrt(jnp.mean(latent * latent, -1, keepdims=True) + epsilon)
        * table_ref[:1, :LAT]
    )
    rope = down[:, LAT:]
    half = rope.shape[-1] // 2
    turned = jnp.concatenate([rope[:, half:], rope[:, :half]], 1)
    cos, sin = LAT + 2 * half, LAT + 4 * half
    rope = rope * table_ref[:, LAT:cos] + turned * table_ref[:, cos:sin]
    latent = latent.astype(bf16).astype(f32)[:, None, :]
    rope = rope.astype(bf16).astype(f32)[:, None, :]
    own = (
        jnp.sum(q_ref[:, :, :LAT].astype(f32) * latent, -1, keepdims=True)
        + jnp.sum(q_ref[:, :, LAT:].astype(f32) * rope, -1, keepdims=True)
    ) * score_scale
    cached = jnp.sum(back_ref[:, :, LAT:].astype(f32), -1, keepdims=True)
    peak = jnp.maximum(own, cached)
    own_prob = jnp.exp(own - peak)
    cached_prob = jnp.exp(cached - peak)
    total_prob = own_prob + cached_prob
    o_ref[...] = (
        back_ref[:, :, :LAT].astype(f32) * (cached_prob / total_prob)
        + latent * (own_prob / total_prob)
    ).astype(bf16)


def merge(everything, table, queries, units):
    seqs, heads, _ = queries.shape
    return pl.pallas_call(
        merge_kernel,
        out_shape=shape((seqs, heads, LAT), bf16),
        in_specs=[VMEM] * 4,
        out_specs=VMEM,
        scratch_shapes=[pltpu.VMEM((seqs, heads, LAT + 128), bf16)],
        compiler_params=PARAMS,
        name="merge",
    )(everything, table, queries, units)


def rope_tables(lengths, half):
    inv_freq = 10000.0 ** (-jnp.arange(half, dtype=f32) / half)
    angles = lengths.astype(f32)[:, None] * inv_freq[None, :]
    cos, sin = jnp.cos(angles), jnp.sin(angles)
    return jnp.concatenate([cos, cos], 1), jnp.concatenate([-sin, sin], 1)


def local(
    hidden,
    moe_gain,
    expert_ids,
    slots,
    affinity,
    w_gate,
    w_up,
    w_down,
    attn_gain,
    w_dkv,
    kv_gain,
    queries,
    cache,
    lengths,
):
    seqs, width = hidden.shape
    peers = lax.axis_size("tp")
    experts = lax.axis_size("ep") * lax.axis_size("mb")
    me = lax.axis_index("tp").astype(jnp.int32).reshape(1)

    def moved(x, k):
        return lax.ppermute(x, "tp", [(i, (i + k) % peers) for i in range(peers)])

    send_rows, combine = route(expert_ids, slots, affinity, hidden, experts)
    arrived = exchange(send_rows, ("ep", "mb"))
    blocks = list(pack(me, w_down[0], cache, queries, moe_gain[None], peers))
    for k in MOVES:
        blocks[k] = moved(blocks[k], k)
    parts = ring(packed_rows(arrived), moved, peers)
    span, heads, keys = cache.shape[1], queries.shape[1], queries.shape[2]
    attended = attend(me, lengths, blocks, seqs // peers, span, heads, keys)
    units = expert_units(me, parts, w_gate[0], w_up[0], attended, blocks)
    all_units = exchange(units, "tp")
    columns = columns_of(blocks, w_down.shape[1], width)
    output = expert_down(me, all_units, columns, experts)
    returned = exchange(output, ("ep", "mb"))
    next_hidden, small = close(returned, combine, hidden, attn_gain[None], w_dkv, peers)
    everything = exchange(small, "tp")
    gain = jnp.broadcast_to(kv_gain, (seqs, LAT))
    table = jnp.concatenate([gain, *rope_tables(lengths, (keys - LAT) // 2)], 1)
    latent_out = merge(everything, table, queries, all_units)
    return (next_hidden, latent_out)


def solution(mesh):
    return jax.shard_map(
        local,
        mesh=mesh,
        in_specs=(
            P(("grp", "ep", "mb"), "tp"),
            P("tp"),
            P(("grp", "ep", "mb"), None),
            P(("grp", "ep", "mb"), None),
            P(("grp", "ep", "mb"), None),
            P(("ep", "mb"), None, "tp"),
            P(("ep", "mb"), None, "tp"),
            P(("ep", "mb"), "tp", None),
            P("tp"),
            P("tp", None),
            P(),
            P(("grp", "ep", "mb"), "tp", None),
            P(("grp", "ep", "mb"), "tp", None),
            P(("grp", "ep", "mb")),
        ),
        out_specs=(P(("grp", "ep", "mb"), "tp"), P(("grp", "ep", "mb"), "tp", None)),
        check_vma=False,
    )
```

```python
import jax
import jax.numpy as jnp
from jax import lax
from jax.experimental import pallas as pl
from jax.experimental.pallas import tpu as pltpu
from jax.sharding import PartitionSpec as P


D = 3584
LAT = 512
CAP = 8
BEFORE = (4, 3, 5)
MOVES = BEFORE + (2, 6, 1, 7)

epsilon = 1e-06
route_scale = 2.5
score_scale = 192.0 ** (-0.5)
f32 = jnp.float32
bf16 = jnp.bfloat16
VMEM = pl.BlockSpec(memory_space=pltpu.VMEM)
SMEM = pl.BlockSpec(memory_space=pltpu.SMEM)
HBM = pl.BlockSpec(memory_space=pltpu.HBM)
PARAMS = pltpu.CompilerParams(vmem_limit_bytes=40 * 1024 * 1024)


def shape(dims, dtype):
    return jax.ShapeDtypeStruct(dims, dtype)


def exchange(x, axis):
    return lax.all_to_all(x, axis, split_axis=0, concat_axis=0, tiled=True)


def in_hbm(x):
    return pltpu.with_memory_space_constraint(x, pltpu.HBM)


def fetch(sources, targets, sems):
    copies = [
        pltpu.make_async_copy(source, target, sems.at[i])
        for i, (source, target) in enumerate(zip(sources, targets))
    ]
    for copy in copies:
        copy.start()
    return copies


def route_into(ids_ref, slots_ref, aff_ref, hid_ref, send_ref, comb_ref):
    experts = send_ref.shape[0]
    top, tokens = ids_ref.shape
    rows = experts * CAP
    slots = slots_ref[...]
    affinity = aff_ref[...]
    weight = route_scale * affinity / jnp.sum(affinity, 0, keepdims=True)
    target = jnp.where(slots < CAP, ids_ref[...] * CAP + slots, -1)
    row = lax.broadcasted_iota(jnp.int32, (rows, tokens), 0)
    pick = jnp.zeros((rows, tokens), f32)
    comb = jnp.zeros((rows, tokens), f32)
    for k in range(top):
        match = target[k : k + 1, :] == row
        pick = jnp.where(match, 1.0, pick)
        comb = jnp.where(match, weight[k : k + 1, :], comb)
    comb_ref[...] = comb
    sent = jnp.dot(pick.astype(bf16), hid_ref[...], preferred_element_type=f32)
    send_ref[...] = sent.reshape(send_ref.shape).astype(bf16)


def gain_of(block, at, width):
    rows = block[at : at + 16, :].astype(f32)
    tiles = (width + 127) // 128
    total = rows[:tiles] + rows[tiles : 2 * tiles] + rows[2 * tiles : 3 * tiles]
    return [total[q : q + 1, : min(128, width - 128 * q)] for q in range(tiles)]


def units_kernel(me_ref, wg_hbm, wu_hbm, att_ref, *refs):
    peers = att_ref.shape[0]
    blocks, parts = refs[:peers], refs[peers : 2 * peers + 1]
    o_ref, w_ref, n_ref, h_ref, sems = refs[2 * peers + 1 :]
    hid = wg_hbm.shape[1]
    copies = fetch((wg_hbm, wu_hbm), (w_ref.at[:, :hid], w_ref.at[:, hid:]), sems)
    _, rows, cols = n_ref.shape
    middle, tiles = peers // 2, cols // 128
    square = jnp.zeros((rows, 1), f32)
    for k in range(peers):
        at = 0
        first = k if k <= middle else k + 1
        for part in parts[first : first + (2 if k == middle else 1)]:
            done = 0
            while done < part.shape[0]:
                tile, row = divmod(at, rows)
                take = min(part.shape[0] - done, (rows if tile < tiles else rows // 2) - row)
                piece = part[done : done + take, :]
                if tile < tiles:
                    n_ref[k, row : row + take, 128 * tile : 128 * (tile + 1)] = piece
                else:
                    n_ref[k, row : row + take, 128 * tiles :] = piece[:, :64]
                    n_ref[k, rows // 2 + row : rows // 2 + row + take, 128 * tiles :] = piece[:, 64:]
                at, done = at + take, done + take
        x = n_ref[k].astype(f32)
        square = square + jnp.sum(x * x, -1, keepdims=True)
        j = lax.rem(me_ref[0] + (peers - k), peers)
        gain = jnp.concatenate(gain_of(blocks[k], blocks[k].shape[0] - 16, cols), 1)
        if k == 0:
            copies[0].wait()
            copies[1].wait()
        part = pl.ds(pl.multiple_of(j * cols, 64), cols)
        both = jnp.dot((x * gain).astype(bf16), w_ref[part, :], preferred_element_type=f32)
        if k == 0:
            h_ref[...] = both
        else:
            h_ref[...] += both
        o_ref[j, rows:, :] = att_ref[k]
    scale = lax.rsqrt(square / D + epsilon)
    gate = h_ref[:, :hid] * scale
    units = (gate / (1.0 + jnp.exp(-gate)) * (h_ref[:, hid:] * scale)).astype(bf16)
    for j in range(peers):
        o_ref[j, :rows, :] = units


def expert_units(me, parts, w_gate, w_up, attended, blocks):
    peers = len(blocks)
    cols, hid = w_gate.shape[0] // peers, w_gate.shape[1]
    rows = parts[0].shape[0] * 128 // cols
    return pl.pallas_call(
        units_kernel,
        out_shape=shape((peers, rows + attended.shape[1], hid), bf16),
        in_specs=[SMEM, HBM, HBM] + [VMEM] * (2 * peers + 2),
        out_specs=VMEM,
        scratch_shapes=[
            pltpu.VMEM((w_gate.shape[0], 2 * hid), bf16),
            pltpu.VMEM((peers, rows, cols), bf16),
            pltpu.VMEM((rows, 2 * hid), f32),
            pltpu.SemaphoreType.DMA((2,)),
        ],
        compiler_params=PARAMS,
        name="units",
    )(me, in_hbm(w_gate), in_hbm(w_up), attended, *blocks, *parts)


def pack_kernel(me_ref, *refs):
    inputs, outs, scratch = refs[:8], refs[8:-11], refs[-11:]
    copies = fetch(inputs, scratch[:8], scratch[10])
    wd_ref, cache_ref, q_ref, gain_ref = scratch[:4]
    tiles_ref, keys_ref = scratch[8:10]
    outs, send_ref, comb_ref = outs[:-2], outs[-2], outs[-1]
    peers = len(outs)
    half, double = tiles_ref.shape[1:]
    width = double // 2
    span, heads, keys = cache_ref.shape[1], q_ref.shape[1], cache_ref.shape[2]
    own = cache_ref.shape[0] // peers
    copies[0].wait()
    for j in range(peers):
        tiles_ref[j, :, :width] = wd_ref[:half, j * width : (j + 1) * width]
        tiles_ref[j, :, width:] = wd_ref[half:, j * width : (j + 1) * width]
    copies[3].wait()
    gain = gain_ref[...]
    first = gain.astype(bf16).astype(f32)
    second = (gain - first).astype(bf16).astype(f32)
    row = lax.broadcasted_iota(jnp.int32, (16, 128), 0)
    packed = jnp.zeros((16, 128), f32)
    tiles = (width + 127) // 128
    for p, value in enumerate((first, second, gain - first - second)):
        for q in range(tiles):
            piece = value[:, 128 * q : min(128 * (q + 1), width)]
            if piece.shape[1] < 128:
                piece = jnp.concatenate([piece, jnp.zeros((1, 128 - piece.shape[1]), f32)], 1)
            packed = jnp.where(row == p * tiles + q, piece, packed)
    packed = packed.astype(bf16)
    copies[1].wait()
    copies[2].wait()
    for k in range(peers):
        to = lax.rem(me_ref[0] + k, peers)
        at = 0
        for t in range(double // 128):
            outs[k][at : at + half, :] = tiles_ref[to, :, 128 * t : 128 * (t + 1)]
            at += half
        for i in range(own):
            keys_ref[:span, i * keys : (i + 1) * keys] = cache_ref[to * own + i]
            keys_ref[span:, i * keys : (i + 1) * keys] = q_ref[to * own + i]
        for t in range(own * keys // 128):
            outs[k][at : at + span + heads, :] = keys_ref[:, 128 * t : 128 * (t + 1)]
            at += span + heads
        outs[k][at : at + 16, :] = packed
    for copy in copies[4:]:
        copy.wait()
    route_into(*scratch[4:8], send_ref, comb_ref)


def pack(me, w_down, cache, queries, gain, expert_ids, slots, affinity, hidden, peers, experts):
    hid, width = w_down.shape[0], w_down.shape[1] // peers
    seqs, span, keys = cache.shape
    own, heads = seqs // peers, queries.shape[1]
    rows = hid * width // 128 + own * (span + heads) * keys // 128 + 16
    inputs = (w_down, cache, queries, gain, expert_ids.T, slots.T, affinity.T, hidden)
    *blocks, send_rows, combine = pl.pallas_call(
        pack_kernel,
        out_shape=tuple(shape((rows, 128), bf16) for _ in range(peers))
        + (shape((experts, CAP, width), bf16), shape((experts * CAP, seqs), f32)),
        in_specs=[SMEM] + [HBM] * len(inputs),
        out_specs=tuple(VMEM for _ in range(peers + 2)),
        scratch_shapes=[pltpu.VMEM(x.shape, x.dtype) for x in inputs]
        + [
            pltpu.VMEM((peers, hid // 2, 2 * width), bf16),
            pltpu.VMEM((span + heads, own * keys), bf16),
            pltpu.SemaphoreType.DMA((len(inputs),)),
        ],
        compiler_params=PARAMS,
        name="pack",
    )(me, *[in_hbm(x) for x in inputs])
    return blocks, send_rows, combine


def rows_kernel(x_ref, o_ref):
    experts, cap, width = x_ref.shape
    rows = experts * cap
    x = x_ref[...].reshape(rows, width)
    tiles = width // 128
    for t in range(tiles):
        o_ref[t * rows : (t + 1) * rows, :] = x[:, 128 * t : 128 * (t + 1)]
    o_ref[tiles * rows :, :64] = x[: rows // 2, 128 * tiles :]
    o_ref[tiles * rows :, 64:] = x[rows // 2 :, 128 * tiles :]


def packed_rows(arrived):
    experts, cap, width = arrived.shape
    return pl.pallas_call(
        rows_kernel,
        out_shape=shape((experts * cap * width // 128, 128), bf16),
        in_specs=[VMEM],
        out_specs=VMEM,
        compiler_params=PARAMS,
        name="rows",
    )(arrived)


def ring(x, moved, peers):
    steps, half = peers // 2, x.shape[0] // 2
    there, back = [x], [x]
    for _ in range(1, steps):
        there.append(moved(there[-1], 1))
        back.append(moved(back[-1], peers - 1))
    upper = moved(there[-1][:half], 1)
    lower = moved(back[-1][half:], peers - 1)
    return there + [upper, lower] + back[:0:-1]


def columns_kernel(*refs):
    blocks, o_ref, w_ref = refs[:-2], refs[-2], refs[-1]
    half, double = w_ref.shape
    width = double // 2
    for k in range(len(blocks)):
        for t in range(double // 128):
            w_ref[:, 128 * t : 128 * (t + 1)] = blocks[k][half * t : half * (t + 1), :]
        o_ref[k, :half, :] = w_ref[:, :width]
        o_ref[k, half:, :] = w_ref[:, width:]


def columns_of(blocks, hid, width):
    return pl.pallas_call(
        columns_kernel,
        out_shape=shape((len(blocks), hid, width), bf16),
        in_specs=[VMEM] * len(blocks),
        out_specs=VMEM,
        scratch_shapes=[pltpu.VMEM((hid // 2, 2 * width), bf16)],
        compiler_params=PARAMS,
        name="columns",
    )(*blocks)


def down_kernel(me_ref, u_ref, w_ref, o_ref):
    peers = u_ref.shape[0]
    experts, cap, width = o_ref.shape
    acc = jnp.zeros((experts * cap, width), f32)
    for k in range(peers):
        group = lax.rem(me_ref[0] + (peers - k), peers)
        acc = acc + jnp.dot(
            u_ref[group, : experts * cap, :], w_ref[k], preferred_element_type=f32
        )
    o_ref[...] = acc.reshape(o_ref.shape).astype(bf16)


def expert_down(me, units, columns, experts):
    return pl.pallas_call(
        down_kernel,
        out_shape=shape((experts, CAP, columns.shape[2]), bf16),
        in_specs=[SMEM, VMEM, VMEM],
        out_specs=VMEM,
        compiler_params=PARAMS,
        name="down",
    )(me, units, columns)


def attend_kernel(me_ref, len_ref, *refs):
    peers = len(refs) - 4
    blocks, (o_ref, m_ref, c_ref, q_ref) = refs[:peers], refs[peers:]
    own, positions, keys = c_ref.shape
    span, heads = positions // peers, q_ref.shape[1] // peers
    me = me_ref[0]
    first = blocks[0].shape[0] - 16 - own * keys // 128 * (span + heads)
    for k in range(peers):
        for t in range(own * keys // 128):
            at = first + t * (span + heads)
            m_ref[:, 128 * t : 128 * (t + 1)] = blocks[k][at : at + span + heads, :]
        for i in range(own):
            c_ref[i, k * span : (k + 1) * span, :] = m_ref[:span, i * keys : (i + 1) * keys]
            q_ref[i, k * heads : (k + 1) * heads, :] = m_ref[span:, i * keys : (i + 1) * keys]
    lane = lax.broadcasted_iota(jnp.int32, (peers * heads, positions), 1)
    block = lax.rem(me + (peers - lane // span), peers)
    position = block * span + lane % span
    for i in range(own):
        live = position < len_ref[me * own + i]
        known = c_ref[i]
        scores = (
            lax.dot_general(
                q_ref[i], known, (((1,), (1,)), ((), ())), preferred_element_type=f32
            )
            * score_scale
        )
        scores = jnp.where(live, scores, -1e30)
        peak = jnp.max(scores, -1, keepdims=True)
        prob = jnp.where(live, jnp.exp(scores - peak), 0.0)
        mass = jnp.sum(prob, -1, keepdims=True)
        out = jnp.dot(prob.astype(bf16), known[:, :LAT], preferred_element_type=f32)
        out = (out / mass).astype(bf16)
        total = peak + jnp.log(mass)
        high = total.astype(bf16).astype(f32)
        middle = (total - high).astype(bf16).astype(f32)
        low = total - high - middle
        tail_lane = lax.broadcasted_iota(jnp.int32, (peers * heads, 128), 1)
        tail = jnp.where(
            tail_lane == 0,
            high,
            jnp.where(tail_lane == 1, middle, jnp.where(tail_lane == 2, low, 0.0)),
        ).astype(bf16)
        for k in range(peers):
            for t in range(LAT // 128 + 1):
                at = (t * own + i) * heads
                piece = tail if t == LAT // 128 else out[:, 128 * t : 128 * (t + 1)]
                o_ref[k, at : at + heads, :] = piece[k * heads : (k + 1) * heads]


def attend(me, lengths, blocks, own, span, heads, keys):
    peers = len(blocks)
    return pl.pallas_call(
        attend_kernel,
        out_shape=shape((peers, own * heads * (LAT // 128 + 1), 128), bf16),
        in_specs=[SMEM, SMEM] + [VMEM] * peers,
        out_specs=VMEM,
        scratch_shapes=[
            pltpu.VMEM((span + heads, own * keys), bf16),
            pltpu.VMEM((own, peers * span, keys), bf16),
            pltpu.VMEM((own, peers * heads, keys), bf16),
        ],
        compiler_params=PARAMS,
        name="attend",
    )(me, lengths, *blocks)


def close_kernel(ret_ref, comb_ref, hid_ref, gain_ref, wdkv_ref, next_ref, small_ref):
    rows = comb_ref.shape[0]
    keys = wdkv_ref.shape[1]
    returned = ret_ref[...].reshape(rows, ret_ref.shape[-1])
    comb = comb_ref[...]
    high = comb.astype(bf16)
    low = (comb - high.astype(f32)).astype(bf16)
    first_dim = (((0,), (0,)), ((), ()))
    moe = lax.dot_general(
        high, returned, first_dim, preferred_element_type=f32
    ) + lax.dot_general(low, returned, first_dim, preferred_element_type=f32)
    result = (hid_ref[...].astype(f32) + moe).astype(bf16)
    next_ref[...] = result
    wide = result.astype(f32)
    square = jnp.sum(wide * wide, -1, keepdims=True)
    first = square.astype(bf16).astype(f32)
    second = (square - first).astype(bf16).astype(f32)
    third = square - first - second
    lane = lax.broadcasted_iota(jnp.int32, (wide.shape[0], small_ref.shape[2] - keys), 1)
    tail = jnp.where(
        lane == 0, first, jnp.where(lane == 1, second, jnp.where(lane == 2, third, 0.0))
    ).astype(bf16)
    down = jnp.dot(
        (wide * gain_ref[...]).astype(bf16), wdkv_ref[...], preferred_element_type=f32
    ).astype(bf16)
    for j in range(small_ref.shape[0]):
        small_ref[j, :, :keys] = down
        small_ref[j, :, keys:] = tail


def close(returned, combine, hidden, gain, w_dkv, peers):
    tokens, width = hidden.shape
    return pl.pallas_call(
        close_kernel,
        out_shape=(
            shape((tokens, width), bf16),
            shape((peers, tokens, w_dkv.shape[1] + 64), bf16),
        ),
        in_specs=[VMEM] * 5,
        out_specs=(VMEM, VMEM),
        compiler_params=PARAMS,
        name="close",
    )(returned, combine, hidden, gain, w_dkv)


def merge_kernel(all_ref, table_ref, q_ref, units_ref, o_ref, back_ref):
    peers = all_ref.shape[0]
    seqs, heads, lanes = back_ref.shape
    own = seqs // peers
    first = units_ref.shape[1] - own * heads * (lanes // 128)
    for j in range(peers):
        for i in range(own):
            for t in range(lanes // 128):
                at = first + (t * own + i) * heads
                back_ref[j * own + i, :, 128 * t : 128 * (t + 1)] = units_ref[
                    j, at : at + heads, :
                ]
    keys = q_ref.shape[-1]
    total = all_ref[0].astype(f32)
    for j in range(1, all_ref.shape[0]):
        total = total + all_ref[j].astype(f32)
    square = jnp.sum(total[:, keys:], -1, keepdims=True)
    down = total[:, :keys] * lax.rsqrt(square / D + epsilon)
    latent = down[:, :LAT]
    latent = (
        latent
        * lax.rsqrt(jnp.mean(latent * latent, -1, keepdims=True) + epsilon)
        * table_ref[:1, :LAT]
    )
    rope = down[:, LAT:]
    half = rope.shape[-1] // 2
    turned = jnp.concatenate([rope[:, half:], rope[:, :half]], 1)
    cos, sin = LAT + 2 * half, LAT + 4 * half
    rope = rope * table_ref[:, LAT:cos] + turned * table_ref[:, cos:sin]
    latent = latent.astype(bf16).astype(f32)[:, None, :]
    rope = rope.astype(bf16).astype(f32)[:, None, :]
    own = (
        jnp.sum(q_ref[:, :, :LAT].astype(f32) * latent, -1, keepdims=True)
        + jnp.sum(q_ref[:, :, LAT:].astype(f32) * rope, -1, keepdims=True)
    ) * score_scale
    cached = jnp.sum(back_ref[:, :, LAT:].astype(f32), -1, keepdims=True)
    peak = jnp.maximum(own, cached)
    own_prob = jnp.exp(own - peak)
    cached_prob = jnp.exp(cached - peak)
    total_prob = own_prob + cached_prob
    o_ref[...] = (
        back_ref[:, :, :LAT].astype(f32) * (cached_prob / total_prob)
        + latent * (own_prob / total_prob)
    ).astype(bf16)


def merge(everything, table, queries, units):
    seqs, heads, _ = queries.shape
    return pl.pallas_call(
        merge_kernel,
        out_shape=shape((seqs, heads, LAT), bf16),
        in_specs=[VMEM] * 4,
        out_specs=VMEM,
        scratch_shapes=[pltpu.VMEM((seqs, heads, LAT + 128), bf16)],
        compiler_params=PARAMS,
        name="merge",
    )(everything, table, queries, units)


def rope_tables(lengths, half):
    inv_freq = 10000.0 ** (-jnp.arange(half, dtype=f32) / half)
    angles = lengths.astype(f32)[:, None] * inv_freq[None, :]
    cos, sin = jnp.cos(angles), jnp.sin(angles)
    return jnp.concatenate([cos, cos], 1), jnp.concatenate([-sin, sin], 1)


def local(
    hidden,
    moe_gain,
    expert_ids,
    slots,
    affinity,
    w_gate,
    w_up,
    w_down,
    attn_gain,
    w_dkv,
    kv_gain,
    queries,
    cache,
    lengths,
):
    seqs, width = hidden.shape
    peers = lax.axis_size("tp")
    experts = lax.axis_size("ep") * lax.axis_size("mb")
    me = lax.axis_index("tp").astype(jnp.int32).reshape(1)

    def moved(x, k):
        return lax.ppermute(x, "tp", [(i, (i + k) % peers) for i in range(peers)])

    blocks, send_rows, combine = pack(
        me,
        w_down[0],
        cache,
        queries,
        moe_gain[None],
        expert_ids,
        slots,
        affinity,
        hidden,
        peers,
        experts,
    )
    arrived = exchange(send_rows, ("ep", "mb"))
    for k in MOVES:
        blocks[k] = moved(blocks[k], k)
    parts = ring(packed_rows(arrived), moved, peers)
    span, heads, keys = cache.shape[1], queries.shape[1], queries.shape[2]
    attended = attend(me, lengths, blocks, seqs // peers, span, heads, keys)
    units = expert_units(me, parts, w_gate[0], w_up[0], attended, blocks)
    all_units = exchange(units, "tp")
    columns = columns_of(blocks, w_down.shape[1], width)
    output = expert_down(me, all_units, columns, experts)
    returned = exchange(output, ("ep", "mb"))
    next_hidden, small = close(returned, combine, hidden, attn_gain[None], w_dkv, peers)
    everything = exchange(small, "tp")
    gain = jnp.broadcast_to(kv_gain, (seqs, LAT))
    table = jnp.concatenate([gain, *rope_tables(lengths, (keys - LAT) // 2)], 1)
    latent_out = merge(everything, table, queries, all_units)
    return (next_hidden, latent_out)


def solution(mesh):
    return jax.shard_map(
        local,
        mesh=mesh,
        in_specs=(
            P(("grp", "ep", "mb"), "tp"),
            P("tp"),
            P(("grp", "ep", "mb"), None),
            P(("grp", "ep", "mb"), None),
            P(("grp", "ep", "mb"), None),
            P(("ep", "mb"), None, "tp"),
            P(("ep", "mb"), None, "tp"),
            P(("ep", "mb"), "tp", None),
            P("tp"),
            P("tp", None),
            P(),
            P(("grp", "ep", "mb"), "tp", None),
            P(("grp", "ep", "mb"), "tp", None),
            P(("grp", "ep", "mb")),
        ),
        out_specs=(P(("grp", "ep", "mb"), "tp"), P(("grp", "ep", "mb"), "tp", None)),
        check_vma=False,
    )
```

```python
import jax
import jax.numpy as jnp
from jax import lax
from jax.experimental import pallas as pl
from jax.experimental.pallas import tpu as pltpu
from jax.sharding import PartitionSpec as P


D = 3584
LAT = 512
CAP = 8
BEFORE = (4, 3, 5)
MOVES = BEFORE + (2, 6, 1, 7)

epsilon = 1e-06
route_scale = 2.5
score_scale = 192.0 ** (-0.5)
f32 = jnp.float32
bf16 = jnp.bfloat16
VMEM = pl.BlockSpec(memory_space=pltpu.VMEM)
SMEM = pl.BlockSpec(memory_space=pltpu.SMEM)
HBM = pl.BlockSpec(memory_space=pltpu.HBM)
PARAMS = pltpu.CompilerParams(vmem_limit_bytes=40 * 1024 * 1024)


def shape(dims, dtype):
    return jax.ShapeDtypeStruct(dims, dtype)


def exchange(x, axis):
    return lax.all_to_all(x, axis, split_axis=0, concat_axis=0, tiled=True)


def in_hbm(x):
    return pltpu.with_memory_space_constraint(x, pltpu.HBM)


def fetch(sources, targets, sems):
    copies = [
        pltpu.make_async_copy(source, target, sems.at[i])
        for i, (source, target) in enumerate(zip(sources, targets))
    ]
    for copy in copies:
        copy.start()
    return copies


def route_into(ids_ref, slots_ref, aff_ref, hid_ref, send_ref, comb_ref):
    experts = send_ref.shape[0]
    top, tokens = ids_ref.shape
    rows = experts * CAP
    slots = slots_ref[...]
    affinity = aff_ref[...]
    weight = route_scale * affinity / jnp.sum(affinity, 0, keepdims=True)
    target = jnp.where(slots < CAP, ids_ref[...] * CAP + slots, -1)
    row = lax.broadcasted_iota(jnp.int32, (rows, tokens), 0)
    pick = jnp.zeros((rows, tokens), f32)
    comb = jnp.zeros((rows, tokens), f32)
    for k in range(top):
        match = target[k : k + 1, :] == row
        pick = jnp.where(match, 1.0, pick)
        comb = jnp.where(match, weight[k : k + 1, :], comb)
    comb_ref[...] = comb
    sent = jnp.dot(pick.astype(bf16), hid_ref[...], preferred_element_type=f32)
    send_ref[...] = sent.reshape(send_ref.shape).astype(bf16)


def gain_of(block, at, width):
    rows = block[at : at + 16, :].astype(f32)
    tiles = (width + 127) // 128
    total = rows[:tiles] + rows[tiles : 2 * tiles] + rows[2 * tiles : 3 * tiles]
    return [total[q : q + 1, : min(128, width - 128 * q)] for q in range(tiles)]


def beside_kernel(wg_hbm, wu_hbm, o_ref, sems):
    hid = wg_hbm.shape[1]
    copies = fetch((wg_hbm, wu_hbm), (o_ref.at[:, :hid], o_ref.at[:, hid:]), sems)
    for copy in copies:
        copy.wait()


def beside(w_gate, w_up):
    rows, hid = w_gate.shape
    return pl.pallas_call(
        beside_kernel,
        out_shape=shape((rows, 2 * hid), bf16),
        in_specs=[HBM, HBM],
        out_specs=VMEM,
        scratch_shapes=[pltpu.SemaphoreType.DMA((2,))],
        compiler_params=PARAMS,
        name="beside",
    )(in_hbm(w_gate), in_hbm(w_up))


def units_kernel(me_ref, w_ref, att_ref, *refs):
    peers = att_ref.shape[0]
    blocks, parts = refs[:peers], refs[peers : 2 * peers + 1]
    o_ref, n_ref, h_ref = refs[2 * peers + 1 :]
    hid = w_ref.shape[1] // 2
    _, rows, cols = n_ref.shape
    middle, tiles = peers // 2, cols // 128
    square = jnp.zeros((rows, 1), f32)
    for k in range(peers):
        at = 0
        first = k if k <= middle else k + 1
        for part in parts[first : first + (2 if k == middle else 1)]:
            done = 0
            while done < part.shape[0]:
                tile, row = divmod(at, rows)
                take = min(part.shape[0] - done, (rows if tile < tiles else rows // 2) - row)
                piece = part[done : done + take, :]
                if tile < tiles:
                    n_ref[k, row : row + take, 128 * tile : 128 * (tile + 1)] = piece
                else:
                    n_ref[k, row : row + take, 128 * tiles :] = piece[:, :64]
                    n_ref[k, rows // 2 + row : rows // 2 + row + take, 128 * tiles :] = piece[:, 64:]
                at, done = at + take, done + take
        x = n_ref[k].astype(f32)
        square = square + jnp.sum(x * x, -1, keepdims=True)
        j = lax.rem(me_ref[0] + (peers - k), peers)
        gain = jnp.concatenate(gain_of(blocks[k], blocks[k].shape[0] - 16, cols), 1)
        part = pl.ds(pl.multiple_of(j * cols, 64), cols)
        both = jnp.dot((x * gain).astype(bf16), w_ref[part, :], preferred_element_type=f32)
        if k == 0:
            h_ref[...] = both
        else:
            h_ref[...] += both
        o_ref[j, rows:, :] = att_ref[k]
    scale = lax.rsqrt(square / D + epsilon)
    gate = h_ref[:, :hid] * scale
    units = (gate / (1.0 + jnp.exp(-gate)) * (h_ref[:, hid:] * scale)).astype(bf16)
    for j in range(peers):
        o_ref[j, :rows, :] = units


def expert_units(me, parts, weights, attended, blocks):
    peers = len(blocks)
    cols, hid = weights.shape[0] // peers, weights.shape[1] // 2
    rows = parts[0].shape[0] * 128 // cols
    return pl.pallas_call(
        units_kernel,
        out_shape=shape((peers, rows + attended.shape[1], hid), bf16),
        in_specs=[SMEM] + [VMEM] * (2 * peers + 3),
        out_specs=VMEM,
        scratch_shapes=[
            pltpu.VMEM((peers, rows, cols), bf16),
            pltpu.VMEM((rows, 2 * hid), f32),
        ],
        compiler_params=PARAMS,
        name="units",
    )(me, weights, attended, *blocks, *parts)


def pack_kernel(me_ref, *refs):
    inputs, outs, scratch = refs[:8], refs[8:-11], refs[-11:]
    copies = fetch(inputs, scratch[:8], scratch[10])
    wd_ref, cache_ref, q_ref, gain_ref = scratch[:4]
    tiles_ref, keys_ref = scratch[8:10]
    outs, send_ref, comb_ref = outs[:-2], outs[-2], outs[-1]
    peers = len(outs)
    half, double = tiles_ref.shape[1:]
    width = double // 2
    span, heads, keys = cache_ref.shape[1], q_ref.shape[1], cache_ref.shape[2]
    own = cache_ref.shape[0] // peers
    copies[0].wait()
    for j in range(peers):
        tiles_ref[j, :, :width] = wd_ref[:half, j * width : (j + 1) * width]
        tiles_ref[j, :, width:] = wd_ref[half:, j * width : (j + 1) * width]
    copies[3].wait()
    gain = gain_ref[...]
    first = gain.astype(bf16).astype(f32)
    second = (gain - first).astype(bf16).astype(f32)
    row = lax.broadcasted_iota(jnp.int32, (16, 128), 0)
    packed = jnp.zeros((16, 128), f32)
    tiles = (width + 127) // 128
    for p, value in enumerate((first, second, gain - first - second)):
        for q in range(tiles):
            piece = value[:, 128 * q : min(128 * (q + 1), width)]
            if piece.shape[1] < 128:
                piece = jnp.concatenate([piece, jnp.zeros((1, 128 - piece.shape[1]), f32)], 1)
            packed = jnp.where(row == p * tiles + q, piece, packed)
    packed = packed.astype(bf16)
    copies[1].wait()
    copies[2].wait()
    for k in range(peers):
        to = lax.rem(me_ref[0] + k, peers)
        at = 0
        for t in range(double // 128):
            outs[k][at : at + half, :] = tiles_ref[to, :, 128 * t : 128 * (t + 1)]
            at += half
        for i in range(own):
            keys_ref[:span, i * keys : (i + 1) * keys] = cache_ref[to * own + i]
            keys_ref[span:, i * keys : (i + 1) * keys] = q_ref[to * own + i]
        for t in range(own * keys // 128):
            outs[k][at : at + span + heads, :] = keys_ref[:, 128 * t : 128 * (t + 1)]
            at += span + heads
        outs[k][at : at + 16, :] = packed
    for copy in copies[4:]:
        copy.wait()
    route_into(*scratch[4:8], send_ref, comb_ref)


def pack(me, w_down, cache, queries, gain, expert_ids, slots, affinity, hidden, peers, experts):
    hid, width = w_down.shape[0], w_down.shape[1] // peers
    seqs, span, keys = cache.shape
    own, heads = seqs // peers, queries.shape[1]
    rows = hid * width // 128 + own * (span + heads) * keys // 128 + 16
    inputs = (w_down, cache, queries, gain, expert_ids.T, slots.T, affinity.T, hidden)
    *blocks, send_rows, combine = pl.pallas_call(
        pack_kernel,
        out_shape=tuple(shape((rows, 128), bf16) for _ in range(peers))
        + (shape((experts, CAP, width), bf16), shape((experts * CAP, seqs), f32)),
        in_specs=[SMEM] + [HBM] * len(inputs),
        out_specs=tuple(VMEM for _ in range(peers + 2)),
        scratch_shapes=[pltpu.VMEM(x.shape, x.dtype) for x in inputs]
        + [
            pltpu.VMEM((peers, hid // 2, 2 * width), bf16),
            pltpu.VMEM((span + heads, own * keys), bf16),
            pltpu.SemaphoreType.DMA((len(inputs),)),
        ],
        compiler_params=PARAMS,
        name="pack",
    )(me, *[in_hbm(x) for x in inputs])
    return blocks, send_rows, combine


def rows_kernel(x_ref, o_ref):
    experts, cap, width = x_ref.shape
    rows = experts * cap
    x = x_ref[...].reshape(rows, width)
    tiles = width // 128
    for t in range(tiles):
        o_ref[t * rows : (t + 1) * rows, :] = x[:, 128 * t : 128 * (t + 1)]
    o_ref[tiles * rows :, :64] = x[: rows // 2, 128 * tiles :]
    o_ref[tiles * rows :, 64:] = x[rows // 2 :, 128 * tiles :]


def packed_rows(arrived):
    experts, cap, width = arrived.shape
    return pl.pallas_call(
        rows_kernel,
        out_shape=shape((experts * cap * width // 128, 128), bf16),
        in_specs=[VMEM],
        out_specs=VMEM,
        compiler_params=PARAMS,
        name="rows",
    )(arrived)


def ring(x, moved, peers):
    steps, half = peers // 2, x.shape[0] // 2
    there, back = [x], [x]
    for _ in range(1, steps):
        there.append(moved(there[-1], 1))
        back.append(moved(back[-1], peers - 1))
    upper = moved(there[-1][:half], 1)
    lower = moved(back[-1][half:], peers - 1)
    return there + [upper, lower] + back[:0:-1]


def columns_kernel(*refs):
    blocks, o_ref, w_ref = refs[:-2], refs[-2], refs[-1]
    half, double = w_ref.shape
    width = double // 2
    for k in range(len(blocks)):
        for t in range(double // 128):
            w_ref[:, 128 * t : 128 * (t + 1)] = blocks[k][half * t : half * (t + 1), :]
        o_ref[k, :half, :] = w_ref[:, :width]
        o_ref[k, half:, :] = w_ref[:, width:]


def columns_of(blocks, hid, width):
    return pl.pallas_call(
        columns_kernel,
        out_shape=shape((len(blocks), hid, width), bf16),
        in_specs=[VMEM] * len(blocks),
        out_specs=VMEM,
        scratch_shapes=[pltpu.VMEM((hid // 2, 2 * width), bf16)],
        compiler_params=PARAMS,
        name="columns",
    )(*blocks)


def down_kernel(me_ref, u_ref, w_ref, o_ref):
    peers = u_ref.shape[0]
    experts, cap, width = o_ref.shape
    acc = jnp.zeros((experts * cap, width), f32)
    for k in range(peers):
        group = lax.rem(me_ref[0] + (peers - k), peers)
        acc = acc + jnp.dot(
            u_ref[group, : experts * cap, :], w_ref[k], preferred_element_type=f32
        )
    o_ref[...] = acc.reshape(o_ref.shape).astype(bf16)


def expert_down(me, units, columns, experts):
    return pl.pallas_call(
        down_kernel,
        out_shape=shape((experts, CAP, columns.shape[2]), bf16),
        in_specs=[SMEM, VMEM, VMEM],
        out_specs=VMEM,
        compiler_params=PARAMS,
        name="down",
    )(me, units, columns)


def attend_kernel(me_ref, len_ref, *refs):
    peers = len(refs) - 4
    blocks, (o_ref, m_ref, c_ref, q_ref) = refs[:peers], refs[peers:]
    own, positions, keys = c_ref.shape
    span, heads = positions // peers, q_ref.shape[1] // peers
    me = me_ref[0]
    first = blocks[0].shape[0] - 16 - own * keys // 128 * (span + heads)
    for k in range(peers):
        for t in range(own * keys // 128):
            at = first + t * (span + heads)
            m_ref[:, 128 * t : 128 * (t + 1)] = blocks[k][at : at + span + heads, :]
        for i in range(own):
            c_ref[i, k * span : (k + 1) * span, :] = m_ref[:span, i * keys : (i + 1) * keys]
            q_ref[i, k * heads : (k + 1) * heads, :] = m_ref[span:, i * keys : (i + 1) * keys]
    lane = lax.broadcasted_iota(jnp.int32, (peers * heads, positions), 1)
    block = lax.rem(me + (peers - lane // span), peers)
    position = block * span + lane % span
    for i in range(own):
        live = position < len_ref[me * own + i]
        known = c_ref[i]
        scores = (
            lax.dot_general(
                q_ref[i], known, (((1,), (1,)), ((), ())), preferred_element_type=f32
            )
            * score_scale
        )
        scores = jnp.where(live, scores, -1e30)
        peak = jnp.max(scores, -1, keepdims=True)
        prob = jnp.where(live, jnp.exp(scores - peak), 0.0)
        mass = jnp.sum(prob, -1, keepdims=True)
        out = jnp.dot(prob.astype(bf16), known[:, :LAT], preferred_element_type=f32)
        out = (out / mass).astype(bf16)
        total = peak + jnp.log(mass)
        high = total.astype(bf16).astype(f32)
        middle = (total - high).astype(bf16).astype(f32)
        low = total - high - middle
        tail_lane = lax.broadcasted_iota(jnp.int32, (peers * heads, 128), 1)
        tail = jnp.where(
            tail_lane == 0,
            high,
            jnp.where(tail_lane == 1, middle, jnp.where(tail_lane == 2, low, 0.0)),
        ).astype(bf16)
        for k in range(peers):
            for t in range(LAT // 128 + 1):
                at = (t * own + i) * heads
                piece = tail if t == LAT // 128 else out[:, 128 * t : 128 * (t + 1)]
                o_ref[k, at : at + heads, :] = piece[k * heads : (k + 1) * heads]


def attend(me, lengths, blocks, own, span, heads, keys):
    peers = len(blocks)
    return pl.pallas_call(
        attend_kernel,
        out_shape=shape((peers, own * heads * (LAT // 128 + 1), 128), bf16),
        in_specs=[SMEM, SMEM] + [VMEM] * peers,
        out_specs=VMEM,
        scratch_shapes=[
            pltpu.VMEM((span + heads, own * keys), bf16),
            pltpu.VMEM((own, peers * span, keys), bf16),
            pltpu.VMEM((own, peers * heads, keys), bf16),
        ],
        compiler_params=PARAMS,
        name="attend",
    )(me, lengths, *blocks)


def close_kernel(ret_ref, comb_ref, hid_ref, gain_ref, wdkv_ref, next_ref, small_ref):
    rows = comb_ref.shape[0]
    keys = wdkv_ref.shape[1]
    returned = ret_ref[...].reshape(rows, ret_ref.shape[-1])
    comb = comb_ref[...]
    high = comb.astype(bf16)
    low = (comb - high.astype(f32)).astype(bf16)
    first_dim = (((0,), (0,)), ((), ()))
    moe = lax.dot_general(
        high, returned, first_dim, preferred_element_type=f32
    ) + lax.dot_general(low, returned, first_dim, preferred_element_type=f32)
    result = (hid_ref[...].astype(f32) + moe).astype(bf16)
    next_ref[...] = result
    wide = result.astype(f32)
    square = jnp.sum(wide * wide, -1, keepdims=True)
    first = square.astype(bf16).astype(f32)
    second = (square - first).astype(bf16).astype(f32)
    third = square - first - second
    lane = lax.broadcasted_iota(jnp.int32, (wide.shape[0], small_ref.shape[2] - keys), 1)
    tail = jnp.where(
        lane == 0, first, jnp.where(lane == 1, second, jnp.where(lane == 2, third, 0.0))
    ).astype(bf16)
    down = jnp.dot(
        (wide * gain_ref[...]).astype(bf16), wdkv_ref[...], preferred_element_type=f32
    ).astype(bf16)
    for j in range(small_ref.shape[0]):
        small_ref[j, :, :keys] = down
        small_ref[j, :, keys:] = tail


def close(returned, combine, hidden, gain, w_dkv, peers):
    tokens, width = hidden.shape
    return pl.pallas_call(
        close_kernel,
        out_shape=(
            shape((tokens, width), bf16),
            shape((peers, tokens, w_dkv.shape[1] + 64), bf16),
        ),
        in_specs=[VMEM] * 5,
        out_specs=(VMEM, VMEM),
        compiler_params=PARAMS,
        name="close",
    )(returned, combine, hidden, gain, w_dkv)


def merge_kernel(all_ref, table_ref, q_ref, units_ref, o_ref, back_ref):
    peers = all_ref.shape[0]
    seqs, heads, lanes = back_ref.shape
    own = seqs // peers
    first = units_ref.shape[1] - own * heads * (lanes // 128)
    for j in range(peers):
        for i in range(own):
            for t in range(lanes // 128):
                at = first + (t * own + i) * heads
                back_ref[j * own + i, :, 128 * t : 128 * (t + 1)] = units_ref[
                    j, at : at + heads, :
                ]
    keys = q_ref.shape[-1]
    total = all_ref[0].astype(f32)
    for j in range(1, all_ref.shape[0]):
        total = total + all_ref[j].astype(f32)
    square = jnp.sum(total[:, keys:], -1, keepdims=True)
    down = total[:, :keys] * lax.rsqrt(square / D + epsilon)
    latent = down[:, :LAT]
    latent = (
        latent
        * lax.rsqrt(jnp.mean(latent * latent, -1, keepdims=True) + epsilon)
        * table_ref[:1, :LAT]
    )
    rope = down[:, LAT:]
    half = rope.shape[-1] // 2
    turned = jnp.concatenate([rope[:, half:], rope[:, :half]], 1)
    cos, sin = LAT + 2 * half, LAT + 4 * half
    rope = rope * table_ref[:, LAT:cos] + turned * table_ref[:, cos:sin]
    latent = latent.astype(bf16).astype(f32)[:, None, :]
    rope = rope.astype(bf16).astype(f32)[:, None, :]
    own = (
        jnp.sum(q_ref[:, :, :LAT].astype(f32) * latent, -1, keepdims=True)
        + jnp.sum(q_ref[:, :, LAT:].astype(f32) * rope, -1, keepdims=True)
    ) * score_scale
    cached = jnp.sum(back_ref[:, :, LAT:].astype(f32), -1, keepdims=True)
    peak = jnp.maximum(own, cached)
    own_prob = jnp.exp(own - peak)
    cached_prob = jnp.exp(cached - peak)
    total_prob = own_prob + cached_prob
    o_ref[...] = (
        back_ref[:, :, :LAT].astype(f32) * (cached_prob / total_prob)
        + latent * (own_prob / total_prob)
    ).astype(bf16)


def merge(everything, table, queries, units):
    seqs, heads, _ = queries.shape
    return pl.pallas_call(
        merge_kernel,
        out_shape=shape((seqs, heads, LAT), bf16),
        in_specs=[VMEM] * 4,
        out_specs=VMEM,
        scratch_shapes=[pltpu.VMEM((seqs, heads, LAT + 128), bf16)],
        compiler_params=PARAMS,
        name="merge",
    )(everything, table, queries, units)


def rope_tables(lengths, half):
    inv_freq = 10000.0 ** (-jnp.arange(half, dtype=f32) / half)
    angles = lengths.astype(f32)[:, None] * inv_freq[None, :]
    cos, sin = jnp.cos(angles), jnp.sin(angles)
    return jnp.concatenate([cos, cos], 1), jnp.concatenate([-sin, sin], 1)


def local(
    hidden,
    moe_gain,
    expert_ids,
    slots,
    affinity,
    w_gate,
    w_up,
    w_down,
    attn_gain,
    w_dkv,
    kv_gain,
    queries,
    cache,
    lengths,
):
    seqs, width = hidden.shape
    peers = lax.axis_size("tp")
    experts = lax.axis_size("ep") * lax.axis_size("mb")
    me = lax.axis_index("tp").astype(jnp.int32).reshape(1)

    def moved(x, k):
        return lax.ppermute(x, "tp", [(i, (i + k) % peers) for i in range(peers)])

    blocks, send_rows, combine = pack(
        me,
        w_down[0],
        cache,
        queries,
        moe_gain[None],
        expert_ids,
        slots,
        affinity,
        hidden,
        peers,
        experts,
    )
    arrived = exchange(send_rows, ("ep", "mb"))
    for k in MOVES:
        blocks[k] = moved(blocks[k], k)
    parts = ring(packed_rows(arrived), moved, peers)
    span, heads, keys = cache.shape[1], queries.shape[1], queries.shape[2]
    attended = attend(me, lengths, blocks, seqs // peers, span, heads, keys)
    units = expert_units(me, parts, beside(w_gate[0], w_up[0]), attended, blocks)
    all_units = exchange(units, "tp")
    columns = columns_of(blocks, w_down.shape[1], width)
    output = expert_down(me, all_units, columns, experts)
    returned = exchange(output, ("ep", "mb"))
    next_hidden, small = close(returned, combine, hidden, attn_gain[None], w_dkv, peers)
    everything = exchange(small, "tp")
    gain = jnp.broadcast_to(kv_gain, (seqs, LAT))
    table = jnp.concatenate([gain, *rope_tables(lengths, (keys - LAT) // 2)], 1)
    latent_out = merge(everything, table, queries, all_units)
    return (next_hidden, latent_out)


def solution(mesh):
    return jax.shard_map(
        local,
        mesh=mesh,
        in_specs=(
            P(("grp", "ep", "mb"), "tp"),
            P("tp"),
            P(("grp", "ep", "mb"), None),
            P(("grp", "ep", "mb"), None),
            P(("grp", "ep", "mb"), None),
            P(("ep", "mb"), None, "tp"),
            P(("ep", "mb"), None, "tp"),
            P(("ep", "mb"), "tp", None),
            P("tp"),
            P("tp", None),
            P(),
            P(("grp", "ep", "mb"), "tp", None),
            P(("grp", "ep", "mb"), "tp", None),
            P(("grp", "ep", "mb")),
        ),
        out_specs=(P(("grp", "ep", "mb"), "tp"), P(("grp", "ep", "mb"), "tp", None)),
        check_vma=False,
    )
```
